128 devices in a mesh: rowa: 2 (over x_hi), rowb: 16 (over z, y), col: 4 (over x_lo, core).
Axes of the slice: x: 4 (x_hi: 2, x_lo: 2; x = x_hi * 2 + x_lo), y: 4, z: 4, core: 2. Of those that a mesh axis runs over, the one named last changes fastest.
Arguments:
- table: float32 [262144, 512], P(('rowa', 'rowb'), 'col'), may hold values from -12 to 12
- start: float32 [16, 512], P(None, 'col'), may hold values from -6 to 6
Outputs:
- right_vectors: float32 [16, 512], P(None, 'col')
- left_images: float32 [16, 262144], P(None, ('rowa', 'rowb'))
- strengths: float32 [16], replicated
The draws below stay inside these ranges and needn't reach their ends.
All inputs are finite; a program needn't handle non-finite values.
Results may differ from the reference program's by a relative error of at most 0.00014.
Values sent between devices are 32-bit elements.
A program may use at most 64 MiB of HBM per device.

```python
import jax
import jax.numpy as jnp
from jax import lax

COLS = 512
BLOCK = 16
STEPS = 8
ROW_DEV = 8192
ROWS = 262144


def draw_table(key, part):
    key_noise, key_scale, key_lead, key_amount = jax.random.split(jax.random.fold_in(key, 17), 4)
    blocks = ROWS // ROW_DEV
    col_scale = jnp.exp(jax.random.uniform(key_scale, (COLS,), jnp.float32, -0.6931472, 0.6931472))
    noise = jax.random.normal(key_noise, (blocks, ROW_DEV, COLS), jnp.float32)
    weight = 0.5
    lead = jax.random.normal(key_lead, (blocks, 1, COLS), jnp.float32) * weight
    amount = jax.random.normal(key_amount, (blocks, ROW_DEV, 1), jnp.float32)
    table = noise * col_scale + amount * lead
    return jnp.clip(table, -12.0, 12.0).reshape(ROWS, COLS)


def steps_of(own_key, extent, shards, smallest, largest):
    level = 1.0
    for position, shards_of in shards:
        draws = jax.random.uniform(jax.random.fold_in(jax.random.fold_in(own_key, 6), position), (shards_of,), jnp.float32, smallest / len(shards), largest / len(shards))
        level = level * jnp.repeat(jnp.exp(draws), extent[position] // shards_of).reshape((-1,) + (1,) * (len(extent) - 1 - position))
    return level


def normal_values(own_key, shape, width, reach, pieces=(), held_as=jnp.bfloat16):
    values = width * jax.random.normal(own_key, shape, jnp.float32)
    if pieces:
        values = values * steps_of(own_key, shape, pieces, -0.22, 0.18)
    return jnp.clip(values, -reach, reach).astype(held_as)


def setup_inputs(seed: int = 0) -> dict:
    streams_of = jax.random.split(jax.random.key(seed), 3)
    table = draw_table(jax.random.fold_in(streams_of[2], 71), 0)
    start = normal_values(streams_of[1], (BLOCK, COLS), 1.0, 6.0, ((1, 4),), jnp.float32)
    return dict(table=table, start=start)


high = lax.Precision.HIGHEST

def reference(table, start):
    vectors = start
    images = None
    lower = None
    for step in range(STEPS):
        images = lax.dot_general(vectors.astype(jnp.float32), table.astype(jnp.float32), (((1,), (1,)), ((), ())), precision=high, preferred_element_type=jnp.float32)
        products = jnp.dot(images.astype(jnp.float32), table.astype(jnp.float32), precision=high, preferred_element_type=jnp.float32)
        gram = lax.dot_general(products.astype(jnp.float32), products.astype(jnp.float32), (((1,), (1,)), ((), ())), precision=high, preferred_element_type=jnp.float32)
        lower = jnp.linalg.cholesky(gram)
        vectors = jax.scipy.linalg.solve_triangular(lower, products, lower=True)
    strengths = jnp.diagonal(lower) / ROWS
    return (vectors, images, strengths)
```

```python
import functools

import jax
import jax.numpy as jnp
from jax import lax
from jax.experimental import pallas as pl
from jax.experimental.pallas import tpu as pltpu
from jax.sharding import PartitionSpec as P

STEPS = 8
MESH = pl.DeviceIdType.MESH
f32 = jnp.float32
bf16 = jnp.bfloat16
CHUNKS = 8
CW = 16


def dot(a, b):
    return lax.dot_general(a, b, (((1,), (0,)), ((), ())), preferred_element_type=f32)


def dot_nt(a, b):
    return lax.dot_general(a, b, (((1,), (1,)), ((), ())), preferred_element_type=f32)


def split2(x):
    h = x.astype(bf16)
    return h, (x - h.astype(f32)).astype(bf16)


def split3(x):
    h = x.astype(bf16)
    r = x - h.astype(f32)
    m = r.astype(bf16)
    return h, m, (r - m.astype(f32)).astype(bf16)


def times_cover(v, g1, g2, g3):
    h, m, l = split3(v)
    a = jnp.concatenate([h, m, l], 0)
    o1, o2, o3 = dot(a, g1[...]), dot(a[:32], g2[...]), dot(h, g3[...])
    return o1[:16] + (o1[16:32] + o2[:16]) + (o1[32:] + o2[16:] + o3)


def outer_gram(p):
    h, m, l = split3(p)
    a = jnp.concatenate([h, m, l], 0)
    o1, o2, o3 = dot_nt(a, h), dot_nt(a[:32], m), dot_nt(h, l)
    return o1[:16] + (o1[16:32] + o2[:16]) + (o1[32:] + o2[16:] + o3)


def orthonormal(gram, p):
    rows = lax.broadcasted_iota(jnp.int32, (16, 128), 0)
    cols = [jnp.broadcast_to(gram[:, k : k + 1], (16, 128)) for k in range(16)]
    tiles = [p[:, 128 * t : 128 * t + 128] for t in range(4)]
    pivots = jnp.zeros((16, 128), f32)
    for k in range(16):
        d = cols[k][k : k + 1, :]
        pivots = jnp.where(rows == k, d, pivots)
        if k < 15:
            m = jnp.where(rows > k, cols[k] * (1.0 / d), 0.0)
            for j in range(k + 1, 16):
                cols[j] = cols[j] - m * cols[j][k : k + 1, :]
            tiles = [t - m * t[k : k + 1, :] for t in tiles]
    s = jnp.sqrt(pivots)
    r = 1.0 / s
    return jnp.concatenate([t * r for t in tiles], 1), s


def kernel(
    rows_total,
    table, start, right_o, left_o, str_o,
    tab, tt, rt, stt, frt, wh, wl, ih, il, rst,
    src, ry, sy, rz, sx, rx, gz, gy,
    g1, g2, g3, img, limg, vs,
    load_s, st_s, st_r, nat_s, nat_r, tq_s, tq_r, ex_s, ex_r, fw_s, fw_r,
    y_s, y_r, z_s, z_r, x_s, x_r, az_s, az_r, ay_s, ay_r,
    im_s, im_r, if_s, if_r, out_s,
):
    ra, rb, c = lax.axis_index("rowa"), lax.axis_index("rowb"), lax.axis_index("col")
    y, z = rb % 4, rb // 4
    core, half = c % 2, c // 2
    mine, other = 2 * half, 2 - 2 * half
    sib, par, dia = c ^ 1, c ^ 2, c ^ 3

    def at_col(k):
        return (ra, rb, k)

    def at_y(d):
        return (ra, z * 4 + (y ^ d), c)

    def at_z(d):
        return (ra, (z ^ d) * 4 + y, c)

    def at_x(da, dc):
        return (ra ^ da, rb, c ^ dc)

    pending = []

    def send(a, b, s, r, dev):
        cp = pltpu.make_async_remote_copy(
            src_ref=a, dst_ref=b, send_sem=s, recv_sem=r, device_id=dev, device_id_type=MESH
        )
        cp.start()
        pending.append(cp)
        return cp

    XP = [(da, dc) for da in range(2) for dc in range(4) if (da, dc) != (0, 0)]

    loads = []
    for i, q in enumerate((other, other + 1, mine, mine + 1)):
        cp = pltpu.make_async_copy(table.at[pl.ds(q * 2048, 2048), :], tab.at[core, q], load_s.at[i])
        cp.start()
        loads.append(cp)

    barrier = pltpu.get_barrier_semaphore()
    for d in (1, 2, 3):
        pl.semaphore_signal(barrier, inc=1, device_id=at_y(d), device_id_type=MESH)
        pl.semaphore_signal(barrier, inc=1, device_id=at_z(d), device_id_type=MESH)
    for da, dc in XP:
        pl.semaphore_signal(barrier, inc=1, device_id=at_x(da, dc), device_id_type=MESH)

    def transpose_quarter(q):
        def body(i, carry):
            o = pl.multiple_of(i * 256, 256)
            tt[q, :, pl.ds(o, 256)] = tab[core, q, pl.ds(o, 256), :].T
            return carry

        lax.fori_loop(0, 8, body, 0)

    exchange = {}

    def send_chunk(j, k):
        w = pl.ds(CW * j, CW)
        exchange[j, k] = send(tt.at[other + k, w], rt.at[k, w], ex_s.at[j, k], ex_r.at[j, k], at_col(par))

    loads[0].wait()
    transpose_quarter(other)
    pl.semaphore_wait(barrier, 13)
    send_chunk(0, 0)
    nat = []
    for i, q in enumerate((mine, mine + 1, other, other + 1)):
        nat.append(
            send(table.at[pl.ds(q * 2048, 2048), :], tab.at[core, q], nat_s.at[i], nat_r.at[i], at_col(sib))
        )
    loads[1].wait()
    transpose_quarter(other + 1)
    for j, k in ((0, 1), (1, 0), (1, 1)):
        send_chunk(j, k)
    starts = [
        send(start, rst.at[c], st_s.at[d - 1], st_r.at[d - 1], at_col(c ^ d)) for d in (1, 2, 3)
    ]
    rst[c] = start[...]
    loads[2].wait()
    transpose_quarter(mine)
    loads[3].wait()
    transpose_quarter(mine + 1)
    tq = send(tt.at[mine + 1 - core], stt, tq_s, tq_r, at_col(sib))

    acc = jnp.zeros((128, 256), f32)
    for i, q in enumerate((mine, mine + 1, other, other + 1)):
        nat[i].wait_recv()

        def body(t, acc, i=i, q=q):
            o = pl.multiple_of(t * 512, 512)
            w = jnp.concatenate([tab[0, q, pl.ds(o, 512), :], tab[1, q, pl.ds(o, 512), :]], 1)
            h, l = split2(w)
            if i < 2:
                wh[i, pl.ds(o, 512), :] = h
                wl[i, pl.ds(o, 512), :] = l
            ah, al = split2(tt[q, :, pl.ds(o, 512)])
            both = dot(jnp.concatenate([ah, al], 0), h)
            return acc + (both[:128] + (both[128:] + dot(ah, l)))

        acc = lax.fori_loop(0, 4, body, acc)
    src[0] = acc.reshape(4, 32, 256)

    def split_rows(block, ref):
        def body(i, carry):
            o = pl.multiple_of(i * 512, 512)
            h, l = split2(ref[:, pl.ds(o, 512)])
            ih[block, :, pl.ds(o, 512)] = h
            il[block, :, pl.ds(o, 512)] = l
            return carry

        lax.fori_loop(0, 4, body, 0)

    cps = {}

    def stage0(s):
        cps["y", s] = [
            send(src.at[s, y ^ d], ry.at[s, d - 1], y_s.at[s, d - 1], y_r.at[s, d - 1], at_y(d)) for d in (1, 2, 3)
        ]

    def stage1(s):
        for cp in cps["y", s]:
            cp.wait_recv()
        sy[s] = (src[s, y] + ry[s, 0] + (ry[s, 1] + ry[s, 2])).reshape(4, 8, 256)
        cps["z", s] = [
            send(sy.at[s, z ^ d], rz.at[s, d - 1], z_s.at[s, d - 1], z_r.at[s, d - 1], at_z(d)) for d in (1, 2, 3)
        ]

    def stage2(s):
        for cp in cps["z", s]:
            cp.wait_recv()
        total = sy[s, z] + rz[s, 0] + (rz[s, 1] + rz[s, 2])
        sx[s] = total
        rx[s, ra, c] = total
        cps["x", s] = [
            send(sx.at[s], rx.at[s, ra, c], x_s.at[s, i], x_r.at[s, i], at_x(da, dc)) for i, (da, dc) in enumerate(XP)
        ]

    def stage3(s):
        for cp in cps["x", s]:
            cp.wait_recv()
        gz[s, z] = rx[s, 0] + rx[s, 1]
        cps["az", s] = [
            send(gz.at[s, z], gz.at[s, z], az_s.at[s, d - 1], az_r.at[s, d - 1], at_z(d)) for d in (1, 2, 3)
        ]

    def stage4(s):
        for cp in cps["az", s]:
            cp.wait_recv()
        cps["ay", s] = [
            send(gz.at[s], gy.at[s, y], ay_s.at[s, d - 1], ay_r.at[s, d - 1], at_y(d)) for d in (1, 2, 3)
        ]
        gy[s, y] = gz[s]

    def stage5(s):
        for cp in cps["ay", s]:
            cp.wait_recv()

    stage0(0)
    split_rows(c, tt.at[mine + core])
    tq.wait_recv()
    split_rows(sib, stt)

    forwards = []
    for j in range(CHUNKS):
        w = pl.ds(CW * j, CW)
        for k in range(2):
            exchange[j, k].wait_recv()
        if j + 2 < CHUNKS:
            for k in range(2):
                exchange[j, k].wait_send()
                pending[:] = [p for p in pending if p is not exchange[j, k]]
                send_chunk(j + 2, k)
        forwards.append(send(rt.at[1 - core, w], frt.at[w], fw_s.at[j], fw_r.at[j], at_col(sib)))
        total = jnp.zeros((CW, 256), f32)
        for k in range(2):

            def body(t, total, k=k, j=j):
                o = pl.multiple_of(t * 1024, 1024)
                ah, al = split2(rt[k, pl.ds(CW * j, CW), pl.ds(o, 1024)])
                h, l = wh[k, pl.ds(o, 1024), :], wl[k, pl.ds(o, 1024), :]
                both = dot(jnp.concatenate([ah, al], 0), h)
                return total + (both[:CW] + (both[CW:] + dot(ah, l)))

            total = lax.fori_loop(0, 2, body, total)
        src[1, CW * j // 32, pl.ds(CW * j % 32, CW), :] = total
        h, l = split2(rt[core, w, :])
        ih[par, w, :] = h
        il[par, w, :] = l
        if j == 1:
            stage1(0)
        if j == 2:
            stage2(0)
        if j == 5:
            stage3(0)
        if j == 6:
            stage4(0)
        if j == 7:
            stage0(1)
            stage5(0)
    for j in range(CHUNKS):
        forwards[j].wait_recv()
    split_rows(dia, frt)

    def block(s, k):
        return gy[s, :, :, k].reshape(128, 256)

    def store_cover(r, k, x):
        for ref, part in zip((g1, g2, g3), split3(x)):
            ref[r : r + 128, k : k + 256] = part

    store_cover(0, 0, block(0, 0))
    store_cover(128, 0, block(0, 1))
    store_cover(256, 256, block(0, 2))
    store_cover(384, 256, block(0, 3))
    for cp in starts:
        cp.wait_recv()
    vectors = jnp.concatenate([rst[k] for k in range(4)], 1)

    stage1(1)
    stage2(1)
    stage3(1)
    stage4(1)
    stage5(1)
    upper = jnp.concatenate([block(1, 2), block(1, 3)], 0)
    below = jnp.concatenate([block(1, 0), block(1, 1)], 0)
    upper = upper + below.T
    store_cover(0, 256, upper[:128])
    store_cover(128, 256, upper[128:])
    below = upper.T
    store_cover(256, 0, below[:128])
    store_cover(384, 0, below[128:])

    def step(vectors):
        products = times_cover(vectors, g1, g2, g3)
        return orthonormal(outer_gram(products), products)

    vectors = lax.fori_loop(0, STEPS - 1, lambda i, v: step(v)[0], vectors)

    vh, vl = split2(vectors)
    vb = jnp.concatenate([vh, vl], 0)
    images = []
    for n in range(2):
        for t in range(2):
            o = 1024 * n + 512 * t
            h = jnp.concatenate([ih[k, :, o : o + 512] for k in range(4)], 0)
            l = jnp.concatenate([il[k, :, o : o + 512] for k in range(4)], 0)
            both = dot(vb, h)
            part = both[:16] + (both[16:] + dot(vh, l))
            img[n, :, 512 * t : 512 * t + 512] = part
            limg[n, c, :, 512 * t : 512 * t + 512] = part
        images.append(
            [
                send(img.at[n], limg.at[n, c], im_s.at[n, i], im_r.at[n, i], at_col(k))
                for i, k in enumerate((par, sib))
            ]
        )
    vectors, diagonal = step(vectors)
    for k in range(4):
        vs[k] = vectors[:, 128 * k : 128 * k + 128]
    right_o[...] = vs[c]
    eye = lax.broadcasted_iota(jnp.int32, (16, 128), 0) == lax.broadcasted_iota(jnp.int32, (16, 128), 1)
    str_o[...] = jnp.sum(jnp.where(eye, diagonal / rows_total, 0.0), 0, keepdims=True)[:, :16]

    outs = []

    def put(n, k):
        cp = pltpu.make_async_copy(
            limg.at[n, k], left_o.at[:, pl.ds(pl.multiple_of(2048 * k + 1024 * n, 1024), 1024)], out_s.at[n, len(outs)]
        )
        cp.start()
        outs.append(cp)

    all_outs = []
    relays = []
    for n in range(2):
        outs = []
        put(n, c)
        images[n][1].wait_recv()
        put(n, sib)
        images[n][0].wait_recv()
        relays.append(send(limg.at[n, par], limg.at[n, par], if_s.at[n], if_r.at[n], at_col(sib)))
        put(n, par)
        all_outs.append(outs)
    for n in range(2):
        outs = all_outs[n]
        relays[n].wait_recv()
        put(n, dia)
    for cp in all_outs[0] + all_outs[1]:
        cp.wait()
    for cp in pending:
        cp.wait_send()


def on_device(rows_total, table, start):
    V, D = pltpu.VMEM, pltpu.SemaphoreType.DMA
    scratch = [
        V((2, 4, 2048, 128), f32),
        V((4, 128, 2048), f32),
        V((2, 128, 2048), f32),
        V((128, 2048), f32),
        V((128, 2048), f32),
        V((2, 2048, 256), bf16),
        V((2, 2048, 256), bf16),
        V((4, 128, 2048), bf16),
        V((4, 128, 2048), bf16),
        V((4, 16, 128), f32),
        V((2, 4, 32, 256), f32),
        V((2, 3, 32, 256), f32),
        V((2, 4, 8, 256), f32),
        V((2, 3, 8, 256), f32),
        V((2, 8, 256), f32),
        V((2, 2, 4, 8, 256), f32),
        V((2, 4, 4, 8, 256), f32),
        V((2, 4, 4, 4, 8, 256), f32),
        V((512, 512), bf16),
        V((512, 512), bf16),
        V((512, 512), bf16),
        V((2, 16, 1024), f32),
        V((2, 4, 16, 1024), f32),
        V((4, 16, 128), f32),
        D((4,)),
        D((3,)), D((3,)),
        D((4,)), D((4,)),
        D, D,
        D((CHUNKS, 2)), D((CHUNKS, 2)),
        D((CHUNKS,)), D((CHUNKS,)),
        D((2, 3)), D((2, 3)),
        D((2, 3)), D((2, 3)),
        D((2, 7)), D((2, 7)),
        D((2, 3)), D((2, 3)),
        D((2, 3)), D((2, 3)),
        D((2, 2)), D((2, 2)),
        D((2,)), D((2,)),
        D((2, 4)),
    ]
    right, left, strengths = pl.pallas_call(
        functools.partial(kernel, rows_total),
        out_shape=[
            jax.ShapeDtypeStruct((16, 128), f32),
            jax.ShapeDtypeStruct((16, 8192), f32),
            jax.ShapeDtypeStruct((1, 16), f32),
        ],
        in_specs=[pl.BlockSpec(memory_space=pl.ANY), pl.BlockSpec(memory_space=pltpu.VMEM)],
        out_specs=[
            pl.BlockSpec(memory_space=pltpu.VMEM),
            pl.BlockSpec(memory_space=pl.ANY),
            pl.BlockSpec(memory_space=pltpu.VMEM),
        ],
        scratch_shapes=scratch,
        compiler_params=pltpu.CompilerParams(
            collective_id=0, has_side_effects=True, vmem_limit_bytes=56 * 1024 * 1024
        ),
    )(table, start)
    return right, left, strengths.reshape(16)


def solution(mesh):
    rows_total = 8192 * mesh.shape["rowa"] * mesh.shape["rowb"]
    return jax.shard_map(
        functools.partial(on_device, rows_total),
        mesh=mesh,
        in_specs=(P(("rowa", "rowb"), "col"), P(None, "col")),
        out_specs=(P(None, "col"), P(None, ("rowa", "rowb")), P()),
        check_vma=False,
    )
```

```python
import functools

import jax
import jax.numpy as jnp
from jax import lax
from jax.experimental import pallas as pl
from jax.experimental.pallas import tpu as pltpu
from jax.sharding import PartitionSpec as P

STEPS = 8
MESH = pl.DeviceIdType.MESH
f32 = jnp.float32
bf16 = jnp.bfloat16
CHUNKS = 8
CW = 16
PIECES = 4
IW = 2048 // PIECES


def dot(a, b):
    return lax.dot_general(a, b, (((1,), (0,)), ((), ())), preferred_element_type=f32)


def dot_nt(a, b):
    return lax.dot_general(a, b, (((1,), (1,)), ((), ())), preferred_element_type=f32)


def split2(x):
    h = x.astype(bf16)
    return h, (x - h.astype(f32)).astype(bf16)


def split3(x):
    h = x.astype(bf16)
    r = x - h.astype(f32)
    m = r.astype(bf16)
    return h, m, (r - m.astype(f32)).astype(bf16)


def times_cover(v, g1, g2, g3):
    h, m, l = split3(v)
    a = jnp.concatenate([h, m, l], 0)
    o1, o2, o3 = dot(a, g1[...]), dot(a[:32], g2[...]), dot(h, g3[...])
    return o1[:16] + (o1[16:32] + o2[:16]) + (o1[32:] + o2[16:] + o3)


def outer_gram(p):
    h, m, l = split3(p)
    a = jnp.concatenate([h, m, l], 0)
    o1, o2, o3 = dot_nt(a, h), dot_nt(a[:32], m), dot_nt(h, l)
    return o1[:16] + (o1[16:32] + o2[:16]) + (o1[32:] + o2[16:] + o3)


def orthonormal(gram, p):
    rows = lax.broadcasted_iota(jnp.int32, (16, 128), 0)
    cols = [jnp.broadcast_to(gram[:, k : k + 1], (16, 128)) for k in range(16)]
    tiles = [p[:, 128 * t : 128 * t + 128] for t in range(4)]
    pivots = jnp.zeros((16, 128), f32)
    for k in range(16):
        d = cols[k][k : k + 1, :]
        pivots = jnp.where(rows == k, d, pivots)
        if k < 15:
            m = jnp.where(rows > k, cols[k] * (1.0 / d), 0.0)
            for j in range(k + 1, 16):
                cols[j] = cols[j] - m * cols[j][k : k + 1, :]
            tiles = [t - m * t[k : k + 1, :] for t in tiles]
    s = jnp.sqrt(pivots)
    r = 1.0 / s
    return jnp.concatenate([t * r for t in tiles], 1), s


def kernel(
    rows_total,
    table, start, right_o, left_o, str_o,
    tab, tt, rt, stt, frt, wh, wl, ih, il, rst,
    d_src, d_ry, d_sy, d_rz, d_sx, d_rx, d_gz, d_gy,
    e_src, e_ry, e_sy, e_rz, e_sx, e_rx, e_gz, e_gy,
    f_src, f_ry, f_sy, f_rz, f_sx, f_rx, f_gz, f_gy,
    t_src, t_ry, t_sy, t_rz, t_sx, t_rx, xg,
    g1, g2, g3, img, limg, vs,
    load_s, st_l, st_s, st_r, nat_s, nat_r, tq_s, tq_r, ex_s, ex_r, e0_s, e0_r, fw_s, fw_r,
    y_s, y_r, z_s, z_r, x_s, x_r, az_s, az_r, ay_s, ay_r,
    im_s, im_r, if_s, if_r,
):
    ra, rb, c = lax.axis_index("rowa"), lax.axis_index("rowb"), lax.axis_index("col")
    y, z = rb % 4, rb // 4
    core, half = c % 2, c // 2
    mine, other = 2 * half, 2 - 2 * half
    sib, par, dia = c ^ 1, c ^ 2, c ^ 3

    def at_col(k):
        return (ra, rb, k)

    def at_y(d):
        return (ra, z * 4 + (y ^ d), c)

    def at_z(d):
        return (ra, (z ^ d) * 4 + y, c)

    def at_x(da, dc):
        return (ra ^ da, rb, c ^ dc)

    pending = []

    def send(a, b, s, r, dev):
        cp = pltpu.make_async_remote_copy(
            src_ref=a, dst_ref=b, send_sem=s, recv_sem=r, device_id=dev, device_id_type=MESH
        )
        cp.start()
        pending.append(cp)
        return cp

    XP = [(da, dc) for da in range(2) for dc in range(4) if (da, dc) != (0, 0)]

    own_start = pltpu.make_async_copy(start, rst.at[c], st_l)

    def load(i, q, o, n):
        cp = pltpu.make_async_copy(
            table.at[pl.ds(q * 2048 + o, n), :], tab.at[core, q, pl.ds(o, n), :], load_s.at[i]
        )
        cp.start()
        return cp

    loads = [load(p, other, 512 * p, 512) for p in range(4)]
    loads += [load(4 + i, q, 0, 2048) for i, q in enumerate((other + 1, mine, mine + 1))]
    own_start.start()

    barrier = pltpu.get_barrier_semaphore()
    for d in (1, 2, 3):
        pl.semaphore_signal(barrier, inc=1, device_id=at_y(d), device_id_type=MESH)
        pl.semaphore_signal(barrier, inc=1, device_id=at_z(d), device_id_type=MESH)
    for da, dc in XP:
        pl.semaphore_signal(barrier, inc=1, device_id=at_x(da, dc), device_id_type=MESH)

    def transpose_rows(q, first, blocks):
        def body(i, carry):
            o = pl.multiple_of(first + i * 256, 256)
            tt[q, :, pl.ds(o, 256)] = tab[core, q, pl.ds(o, 256), :].T
            return carry

        lax.fori_loop(0, blocks, body, 0)

    exchange = {}

    def send_chunk(j, k):
        w = pl.ds(CW * j, CW)
        exchange[j, k] = [send(tt.at[other + k, w], rt.at[k, w], ex_s.at[j, k], ex_r.at[j, k], at_col(par))]

    exchange[0, 0] = []
    for p in range(4):
        loads[p].wait()
        transpose_rows(other, 512 * p, 2)
        if p == 0:
            pl.semaphore_wait(barrier, 13)
        o = pl.ds(512 * p, 512)
        exchange[0, 0].append(
            send(tt.at[other, :CW, o], rt.at[0, :CW, o], e0_s.at[p], e0_r.at[p], at_col(par))
        )
    nat = []
    for i, q in enumerate((mine, mine + 1, other, other + 1)):
        nat.append(
            send(table.at[pl.ds(q * 2048, 2048), :], tab.at[core, q], nat_s.at[i], nat_r.at[i], at_col(sib))
        )
    loads[4].wait()
    transpose_rows(other + 1, 0, 8)
    for j, k in ((0, 1), (1, 0), (1, 1)):
        send_chunk(j, k)
    own_start.wait()
    starts = [
        send(rst.at[c], rst.at[c], st_s.at[d - 1], st_r.at[d - 1], at_col(c ^ d)) for d in (1, 2, 3)
    ]
    loads[5].wait()
    transpose_rows(mine, 0, 8)
    loads[6].wait()
    transpose_rows(mine + 1, 0, 8)
    tq = send(tt.at[mine + 1 - core], stt, tq_s, tq_r, at_col(sib))

    acc = jnp.zeros((128, 256), f32)
    for i, q in enumerate((mine, mine + 1, other, other + 1)):
        nat[i].wait_recv()

        def body(t, acc, i=i, q=q):
            o = pl.multiple_of(t * 512, 512)
            w = jnp.concatenate([tab[0, q, pl.ds(o, 512), :], tab[1, q, pl.ds(o, 512), :]], 1)
            h, l = split2(w)
            if i < 2:
                wh[i, pl.ds(o, 512), :] = h
                wl[i, pl.ds(o, 512), :] = l
            ah, al = split2(tt[q, :, pl.ds(o, 512)])
            both = dot(jnp.concatenate([ah, al], 0), h)
            return acc + (both[:128] + (both[128:] + dot(ah, l)))

        acc = lax.fori_loop(0, 4, body, acc)
    d_src[...] = acc.reshape(4, 4, 8, 256)

    def split_rows(block, ref):
        def body(i, carry):
            o = pl.multiple_of(i * 512, 512)
            h, l = split2(ref[:, pl.ds(o, 512)])
            ih[block, :, pl.ds(o, 512)] = h
            il[block, :, pl.ds(o, 512)] = l
            return carry

        lax.fori_loop(0, 4, body, 0)

    def sends(pairs, s, r, devs):
        return [send(a, b, s.at[i], r.at[i], dev) for i, ((a, b), dev) in enumerate(zip(pairs, devs))]

    def arrived(copies):
        for cp in copies:
            cp.wait_recv()

    ys, zs = [at_y(d) for d in (1, 2, 3)], [at_z(d) for d in (1, 2, 3)]
    xs = [at_x(da, dc) for da, dc in XP]

    def scattered(g, src, ry, sy, rz, sx, rx, gz, gy):
        hold = {}

        def stage0():
            hold["y"] = sends([(src.at[y ^ d], ry.at[d - 1]) for d in (1, 2, 3)], y_s.at[g], y_r.at[g], ys)

        def stage1():
            arrived(hold["y"])
            sy[...] = src[y] + ry[0] + (ry[1] + ry[2])
            hold["z"] = sends([(sy.at[z ^ d], rz.at[d - 1]) for d in (1, 2, 3)], z_s.at[g], z_r.at[g], zs)

        def stage2():
            arrived(hold["z"])
            total = sy[z] + rz[0] + (rz[1] + rz[2])
            sx[...] = total
            rx[ra, c] = total
            hold["x"] = sends([(sx, rx.at[ra, c])] * 7, x_s.at[g], x_r.at[g], xs)

        def stage3():
            arrived(hold["x"])
            gz[z] = rx[0] + rx[1]
            hold["az"] = sends([(gz.at[z], gz.at[z])] * 3, az_s.at[g], az_r.at[g], zs)

        def stage4():
            arrived(hold["az"])
            hold["ay"] = sends([(gz, gy.at[y])] * 3, ay_s.at[g], ay_r.at[g], ys)
            gy[y] = gz[...]

        def stage5():
            arrived(hold["ay"])

        return stage0, stage1, stage2, stage3, stage4, stage5

    D = scattered(0, d_src, d_ry, d_sy, d_rz, d_sx, d_rx, d_gz, d_gy)
    E = scattered(1, e_src, e_ry, e_sy, e_rz, e_sx, e_rx, e_gz, e_gy)

    def f0():
        return sends([(f_src.at[y ^ d], f_ry.at[d - 1]) for d in (1, 2, 3)], y_s.at[2], y_r.at[2], ys)

    def f1(cps):
        arrived(cps)
        total = f_src[y] + f_ry[0] + (f_ry[1] + f_ry[2])
        f_sy[...] = total
        f_rz[z] = total
        return sends([(f_sy, f_rz.at[z])] * 3, z_s.at[2], z_r.at[2], zs)

    def f2(cps):
        arrived(cps)
        total = (f_rz[0] + f_rz[1]) + (f_rz[2] + f_rz[3])
        f_sx[...] = total
        f_rx[ra, c] = total
        return sends([(f_sx, f_rx.at[ra, c])] * 7, x_s.at[2], x_r.at[2], xs)

    def f3(cps):
        arrived(cps)
        f_gz[...] = f_rx[0] + f_rx[1]
        out = sends([(f_gz, f_gy.at[y])] * 3, ay_s.at[2], ay_r.at[2], ys)
        f_gy[y] = f_gz[...]
        return out

    def t0():
        t_ry[y] = t_src[...]
        return sends([(t_src, t_ry.at[y])] * 3, y_s.at[3], y_r.at[3], ys)

    def t1(cps):
        arrived(cps)
        total = (t_ry[0] + t_ry[1]) + (t_ry[2] + t_ry[3])
        t_sy[...] = total
        t_rz[z] = total
        return sends([(t_sy, t_rz.at[z])] * 3, z_s.at[3], z_r.at[3], zs)

    def t2(cps):
        arrived(cps)
        total = (t_rz[0] + t_rz[1]) + (t_rz[2] + t_rz[3])
        t_sx[...] = total
        t_rx[ra, c] = total
        return sends([(t_sx, t_rx.at[ra, c])] * 7, x_s.at[3], x_r.at[3], xs)

    D[0]()
    split_rows(c, tt.at[mine + core])
    tq.wait_recv()
    split_rows(sib, stt)

    def chunk_half(j, k, length):
        w = pl.ds(CW * j, CW)

        def body(t, total):
            o = pl.multiple_of(t * length, length)
            ah, al = split2(rt[k, w, pl.ds(o, length)])
            h, l = wh[k, pl.ds(o, length), :], wl[k, pl.ds(o, length), :]
            both = dot(jnp.concatenate([ah, al], 0), h)
            return total + (both[:CW] + (both[CW:] + dot(ah, l)))

        zero = jnp.zeros((CW, 256), f32)
        return body(0, zero) if length == 2048 else lax.fori_loop(0, 2048 // length, body, zero)

    def store_cover(r, k, x):
        for ref, part in zip((g1, g2, g3), split3(x)):
            ref[r : r + 128, k : k + 256] = part

    forwards = []
    for j in range(CHUNKS):
        w = pl.ds(CW * j, CW)
        last = j == CHUNKS - 1
        arrived(exchange[j, 0])
        total = chunk_half(j, 0, 1024)
        arrived(exchange[j, 1])
        if j == 2:
            D[2]()
        if j == 5:
            E[2]()
        if j + 2 < CHUNKS:
            for k in range(2):
                for cp in exchange[j, k]:
                    cp.wait_send()
                    pending[:] = [p for p in pending if p is not cp]
                send_chunk(j + 2, k)
        total = total + chunk_half(j, 1, 2048 if last else 1024)
        if j < 4:
            for i in range(2):
                for n in range(2):
                    e_src[j, 2 * i + n] = total[8 * i : 8 * i + 8, 128 * n : 128 * n + 128]
        elif j < 7:
            for i in range(2):
                for n in range(2):
                    u = (2 * (j - 4) + i) * 2 + n
                    f_src[u // 3, u % 3] = total[8 * i : 8 * i + 8, 128 * n : 128 * n + 128]
        else:
            t_src[...] = total
            tail = t0()
        forwards.append(send(rt.at[1 - core, w], frt.at[w], fw_s.at[j], fw_r.at[j], at_col(sib)))
        h, l = split2(rt[core, w, :])
        ih[par, w, :] = h
        il[par, w, :] = l
        if j == 1:
            D[1]()
        if j == 3:
            E[0]()
        if j == 4:
            D[3]()
            E[1]()
            D[4]()
        if j == 6:
            middle = f0()
            E[3]()
            D[5]()
            for k in range(4):
                store_cover(128 * k, 256 * (k // 2), d_gy[:, :, k].reshape(128, 256))
            E[4]()
            middle = f1(middle)
    middle = f2(middle)
    tail = t1(tail)
    middle = f3(middle)
    E[5]()
    for k in range(4):
        for t in range(4):
            for i in range(2):
                for n in range(2):
                    xg[k, 16 * t + 8 * i : 16 * t + 8 * i + 8, 128 * n : 128 * n + 128] = e_gy[t, 2 * i + n, k]
    tail = t2(tail)
    arrived(forwards)
    split_rows(dia, frt)
    arrived(starts)
    vectors = jnp.concatenate([rst[k] for k in range(4)], 1)
    arrived(middle)
    for k in range(4):
        for u in range(12):
            r = 64 + 8 * (u // 2)
            xg[k, r : r + 8, 128 * (u % 2) : 128 * (u % 2) + 128] = f_gy[u // 3, k, u % 3]
    arrived(tail)
    for k in range(4):
        xg[k, 112:128, :] = t_rx[0, k] + t_rx[1, k]
    upper = xg[2:4].reshape(256, 256) + xg[0:2].reshape(256, 256).T
    store_cover(0, 256, upper[:128])
    store_cover(128, 256, upper[128:])
    below = upper.T
    store_cover(256, 0, below[:128])
    store_cover(384, 0, below[128:])

    def step(vectors):
        products = times_cover(vectors, g1, g2, g3)
        return orthonormal(outer_gram(products), products)

    vectors = lax.fori_loop(0, STEPS - 1, lambda i, v: step(v)[0], vectors)

    vh, vl = split2(vectors)
    vb = jnp.concatenate([vh, vl], 0)
    images = []
    for n in range(PIECES):
        o = pl.ds(IW * n, IW)
        h = jnp.concatenate([ih[k, :, o] for k in range(4)], 0)
        l = jnp.concatenate([il[k, :, o] for k in range(4)], 0)
        both = dot(vb, h)
        part = both[:16] + (both[16:] + dot(vh, l))
        img[n] = part
        limg[n, c] = part
        images.append(
            [send(img.at[n], limg.at[n, c], im_s.at[n, i], im_r.at[n, i], at_col(k)) for i, k in enumerate((par, sib))]
        )
    vectors, diagonal = step(vectors)
    for k in range(4):
        vs[k] = vectors[:, 128 * k : 128 * k + 128]
    right_o[...] = vs[c]
    eye = lax.broadcasted_iota(jnp.int32, (16, 128), 0) == lax.broadcasted_iota(jnp.int32, (16, 128), 1)
    str_o[...] = jnp.sum(jnp.where(eye, diagonal / rows_total, 0.0), 0, keepdims=True)[:, :16]

    relays = []
    for n in range(PIECES):
        images[n][0].wait_recv()
        relays.append(send(limg.at[n, par], limg.at[n, par], if_s.at[n], if_r.at[n], at_col(sib)))
    for n in range(PIECES):
        images[n][1].wait_recv()
        relays[n].wait_recv()
        for k in range(4):
            left_o[:, 2048 * k + IW * n : 2048 * k + IW * n + IW] = limg[n, k]
    for cp in pending:
        cp.wait_send()


def write_out(a, b, d, ao, bo, do, sem):
    copies = [pltpu.make_async_copy(x, o, sem.at[i]) for i, (x, o) in enumerate(((a, ao), (b, bo), (d, do)))]
    for cp in copies:
        cp.start()
    for cp in copies:
        cp.wait()


def scattered_scratch(*unit):
    V = pltpu.VMEM
    return [
        V((4, 4, *unit), f32),
        V((3, 4, *unit), f32),
        V((4, *unit), f32),
        V((3, *unit), f32),
        V(unit, f32),
        V((2, 4, *unit), f32),
        V((4, 4, *unit), f32),
        V((4, 4, 4, *unit), f32),
    ]


def on_device(rows_total, table, start):
    V, D = pltpu.VMEM, pltpu.SemaphoreType.DMA
    scratch = [
        V((2, 4, 2048, 128), f32),
        V((4, 128, 2048), f32),
        V((2, 128, 2048), f32),
        V((128, 2048), f32),
        V((128, 2048), f32),
        V((2, 2048, 256), bf16),
        V((2, 2048, 256), bf16),
        V((4, 128, 2048), bf16),
        V((4, 128, 2048), bf16),
        V((4, 16, 128), f32),
        *scattered_scratch(8, 256),
        *scattered_scratch(8, 128),
        V((4, 3, 8, 128), f32),
        V((3, 3, 8, 128), f32),
        V((3, 8, 128), f32),
        V((4, 3, 8, 128), f32),
        V((3, 8, 128), f32),
        V((2, 4, 3, 8, 128), f32),
        V((4, 3, 8, 128), f32),
        V((4, 4, 3, 8, 128), f32),
        V((16, 256), f32),
        V((4, 16, 256), f32),
        V((16, 256), f32),
        V((4, 16, 256), f32),
        V((16, 256), f32),
        V((2, 4, 16, 256), f32),
        V((4, 128, 256), f32),
        V((512, 512), bf16),
        V((512, 512), bf16),
        V((512, 512), bf16),
        V((PIECES, 16, IW), f32),
        V((PIECES, 4, 16, IW), f32),
        V((4, 16, 128), f32),
        D((7,)),
        D, D((3,)), D((3,)),
        D((4,)), D((4,)),
        D, D,
        D((CHUNKS, 2)), D((CHUNKS, 2)),
        D((4,)), D((4,)),
        D((CHUNKS,)), D((CHUNKS,)),
        D((4, 3)), D((4, 3)),
        D((4, 3)), D((4, 3)),
        D((4, 7)), D((4, 7)),
        D((2, 3)), D((2, 3)),
        D((3, 3)), D((3, 3)),
        D((PIECES, 2)), D((PIECES, 2)),
        D((PIECES,)), D((PIECES,)),
    ]
    table, start = (pltpu.with_memory_space_constraint(x, pltpu.HBM) for x in (table, start))
    results = pl.pallas_call(
        functools.partial(kernel, rows_total),
        out_shape=[V((16, 128), f32), V((16, 8192), f32), V((1, 16), f32)],
        in_specs=[pl.BlockSpec(memory_space=pltpu.HBM)] * 2,
        out_specs=[pl.BlockSpec(memory_space=V)] * 3,
        scratch_shapes=scratch,
        compiler_params=pltpu.CompilerParams(
            collective_id=0, has_side_effects=True, vmem_limit_bytes=48 * 1024 * 1024
        ),
    )(table, start)
    right, left, strengths = pl.pallas_call(
        write_out,
        out_shape=[jax.ShapeDtypeStruct(x.shape, f32) for x in results],
        in_specs=[pl.BlockSpec(memory_space=V)] * 3,
        out_specs=[pl.BlockSpec(memory_space=pl.ANY)] * 3,
        scratch_shapes=[D((3,))],
        compiler_params=pltpu.CompilerParams(vmem_limit_bytes=1024 * 1024),
    )(*results)
    return right, left, strengths.reshape(16)


def solution(mesh):
    rows_total = 8192 * mesh.shape["rowa"] * mesh.shape["rowb"]
    return jax.shard_map(
        functools.partial(on_device, rows_total),
        mesh=mesh,
        in_specs=(P(("rowa", "rowb"), "col"), P(None, "col")),
        out_specs=(P(None, "col"), P(None, ("rowa", "rowb")), P()),
        check_vma=False,
    )
```

```python
import functools
import math

import jax
import jax.numpy as jnp
from jax import lax
from jax.experimental import pallas as pl
from jax.experimental.pallas import tpu as pltpu
from jax.sharding import PartitionSpec as P

STEPS = 8
MESH = pl.DeviceIdType.MESH
f32 = jnp.float32
bf16 = jnp.bfloat16
WIDTHS = (16, 16, 16, 16, 16, 16, 16, 8, 8)
CHUNKS = len(WIDTHS)
PIECES = 8
IW = 2048 // PIECES


def dot(a, b):
    return lax.dot_general(a, b, (((1,), (0,)), ((), ())), preferred_element_type=f32)


def dot_nt(a, b):
    return lax.dot_general(a, b, (((1,), (1,)), ((), ())), preferred_element_type=f32)


def split2(x):
    h = x.astype(bf16)
    return h, (x - h.astype(f32)).astype(bf16)


def split3(x):
    h = x.astype(bf16)
    r = x - h.astype(f32)
    m = r.astype(bf16)
    return h, m, (r - m.astype(f32)).astype(bf16)


def times_cover(v, g1, g2, g3):
    h, m, l = split3(v)
    a = jnp.concatenate([h, m, l], 0)
    o1, o2, o3 = dot(a, g1[...]), dot(a[:32], g2[...]), dot(h, g3[...])
    return o1[:16] + (o1[16:32] + o2[:16]) + (o1[32:] + o2[16:] + o3)


def outer_gram(p):
    h, m, l = split3(p)
    a = jnp.concatenate([h, m, l], 0)
    o1, o2, o3 = dot_nt(a, h), dot_nt(a[:32], m), dot_nt(h, l)
    return o1[:16] + (o1[16:32] + o2[:16]) + (o1[32:] + o2[16:] + o3)


def orthonormal(gram, p):
    rows = lax.broadcasted_iota(jnp.int32, (16, 128), 0)
    cols = [jnp.broadcast_to(gram[:, k : k + 1], (16, 128)) for k in range(16)]
    tiles = [p[:, 128 * t : 128 * t + 128] for t in range(4)]
    pivots = jnp.zeros((16, 128), f32)
    for k in range(16):
        d = cols[k][k : k + 1, :]
        pivots = jnp.where(rows == k, d, pivots)
        if k < 15:
            m = jnp.where(rows > k, cols[k] * (1.0 / d), 0.0)
            for j in range(k + 1, 16):
                cols[j] = cols[j] - m * cols[j][k : k + 1, :]
            tiles = [t - m * t[k : k + 1, :] for t in tiles]
    s = jnp.sqrt(pivots)
    r = 1.0 / s
    return jnp.concatenate([t * r for t in tiles], 1), s


def kernel(
    rows_total,
    table, start, right_o, left_o, str_o,
    tab, tt, rt, stt, frt, wh, wl, ih, il, rst,
    d_src, d_ry, d_sy, d_rz, d_sx, d_rx, d_gz, d_gy,
    e_src, e_ry, e_sy, e_rz, e_sx, e_rx, e_gz, e_gy,
    f_src, f_ry, f_sy, f_rz, f_sx, f_rx, f_gz, f_gy,
    t_src, t_ry, t_sy, t_rz, t_sx, t_rx, xg,
    g1, g2, g3, img, limg, vs,
    load_s, st_l, st_r, nat_s, nat_r, tq_s, tq_r, ex_s, ex_r, fw_s, fw_r,
    all_s, y_r, z_r, x_r, az_r, ay_r, pair_r,
    im_s, im_r, if_s, if_r,
):
    ra, rb, c = lax.axis_index("rowa"), lax.axis_index("rowb"), lax.axis_index("col")
    y, z = rb % 4, rb // 4
    core, half = c % 2, c // 2
    mine, other = 2 * half, 2 - 2 * half
    sib, par, dia = c ^ 1, c ^ 2, c ^ 3

    def at_col(k):
        return (ra, rb, k)

    def at_y(d):
        return (ra, z * 4 + (y ^ d), c)

    def at_z(d):
        return (ra, (z ^ d) * 4 + y, c)

    def at_x(da, dc):
        return (ra ^ da, rb, c ^ dc)

    pending = []

    def send(a, b, s, r, dev):
        cp = pltpu.make_async_remote_copy(
            src_ref=a, dst_ref=b, send_sem=s, recv_sem=r, device_id=dev, device_id_type=MESH
        )
        cp.start()
        pending.append(cp)
        return cp

    def send_apart(*args):
        cp = send(*args)
        pending.pop()
        return cp

    class Waits:
        def __init__(self, whole, s, r):
            self.whole, self.s, self.r = whole, s, r

        def wait_send(self):
            pltpu.make_async_copy(self.whole, self.whole, self.s).wait()

        def wait_recv(self):
            pltpu.make_async_copy(self.whole, self.whole, self.r).wait()

    sent = [0]

    def sends(pairs, r, devs, whole):
        for (a, b), dev in zip(pairs, devs, strict=True):
            send_apart(a, b, all_s, r, dev)
        sent[0] += math.prod(whole.shape) // 1024
        return [Waits(whole, all_s, r)]

    three, seven = pl.ds(0, 3), pl.ds(0, 7)
    spot, spot2 = ra * 4 + c, ra * 2 + half
    pair = [at_col(sib)]

    def arrived(copies):
        for cp in copies:
            cp.wait_recv()

    XP = [(da, dc) for da in range(2) for dc in range(4) if (da, dc) != (0, 0)]

    own_start = pltpu.make_async_copy(start, rst.at[c], st_l)

    def load(i, q, o, n):
        cp = pltpu.make_async_copy(
            table.at[pl.ds(q * 2048 + o, n), :], tab.at[core, q, pl.ds(o, n), :], load_s.at[i]
        )
        cp.start()
        return cp

    loads = [load(p, other, 512 * p, 512) for p in range(4)]
    loads += [load(4 + i, q, 0, 2048) for i, q in enumerate((other + 1, mine, mine + 1))]
    own_start.start()

    barrier = pltpu.get_barrier_semaphore()
    for d in (1, 2, 3):
        pl.semaphore_signal(barrier, inc=1, device_id=at_y(d), device_id_type=MESH)
        pl.semaphore_signal(barrier, inc=1, device_id=at_z(d), device_id_type=MESH)
    for da, dc in XP:
        pl.semaphore_signal(barrier, inc=1, device_id=at_x(da, dc), device_id_type=MESH)

    def transpose_rows(q, first, blocks):
        def body(i, carry):
            o = pl.multiple_of(first + i * 256, 256)
            tt[q, :, pl.ds(o, 256)] = tab[core, q, pl.ds(o, 256), :].T
            return carry

        lax.fori_loop(0, blocks, body, 0)

    def columns(j):
        return pl.ds(sum(WIDTHS[:j]), WIDTHS[j])

    exchange = {}

    def send_chunk(j, k):
        w = columns(j)
        if (j, k) == (CHUNKS - 1, 1):
            halves = [(ex_s, ex_r.at[j + i, k], pl.ds(1024 * i, 1024)) for i in range(2)]
            exchange[j, k] = [
                send_apart(tt.at[other + k, w, o], rt.at[k, w, o], s, r, at_col(par)) for s, r, o in halves
            ]
            return
        exchange[j, k] = [send_apart(tt.at[other + k, w], rt.at[k, w], ex_s, ex_r.at[j, k], at_col(par))]

    for p in range(4):
        loads[p].wait()
        transpose_rows(other, 512 * p, 2)
        if p == 0:
            pl.semaphore_wait(barrier, 13)
        o = pl.ds(512 * p, 512)
        send_apart(tt.at[other, columns(0), o], rt.at[0, columns(0), o], ex_s, ex_r.at[0, 0], at_col(par))
    whole = rt.at[0, columns(0)]
    exchange[0, 0] = [Waits(whole, ex_s, ex_r.at[0, 0])]
    nat = []
    for i, q in enumerate((mine, mine + 1, other, other + 1)):
        nat.append(
            send_apart(table.at[pl.ds(q * 2048, 2048), :], tab.at[core, q], nat_s, nat_r.at[i], at_col(sib))
        )
    pending.append(Waits(tab.at[0], nat_s, nat_s))
    loads[4].wait()
    transpose_rows(other + 1, 0, 8)
    for j, k in ((0, 1), (1, 0), (1, 1)):
        send_chunk(j, k)
    own_start.wait()
    starts = sends([(rst.at[c], rst.at[c])] * 3, st_r, [at_col(c ^ d) for d in (1, 2, 3)], rst.at[three])
    loads[5].wait()
    transpose_rows(mine, 0, 8)
    loads[6].wait()
    transpose_rows(mine + 1, 0, 8)
    tq = send(tt.at[mine + 1 - core], stt, tq_s, tq_r, at_col(sib))

    acc = jnp.zeros((128, 256), f32)
    for i, q in enumerate((mine, mine + 1, other, other + 1)):
        nat[i].wait_recv()

        def body(t, acc, i=i, q=q):
            o = pl.multiple_of(t * 512, 512)
            w = jnp.concatenate([tab[0, q, pl.ds(o, 512), :], tab[1, q, pl.ds(o, 512), :]], 1)
            h, l = split2(w)
            if i < 2:
                wh[i, pl.ds(o, 512), :] = h
                wl[i, pl.ds(o, 512), :] = l
            ah, al = split2(tt[q, :, pl.ds(o, 512)])
            both = dot(jnp.concatenate([ah, al], 0), h)
            return acc + (both[:128] + (both[128:] + dot(ah, l)))

        acc = lax.fori_loop(0, 4, body, acc)
    d_src[...] = acc.reshape(4, 4, 8, 256)

    def split_rows(block, ref):
        def body(i, carry):
            o = pl.multiple_of(i * 512, 512)
            h, l = split2(ref[:, pl.ds(o, 512)])
            ih[block, :, pl.ds(o, 512)] = h
            il[block, :, pl.ds(o, 512)] = l
            return carry

        lax.fori_loop(0, 4, body, 0)

    ys, zs = [at_y(d) for d in (1, 2, 3)], [at_z(d) for d in (1, 2, 3)]
    xs = [at_x(da, dc) for da, dc in XP]
    xs2 = [at_x(da, dc) for da, dc in ((0, 2), (1, 0), (1, 2))]

    def scattered(g, src, ry, sy, rz, sx, rx, gz, gy):
        hold = {}

        def stage0():
            hold["y"] = sends([(src.at[y ^ d], ry.at[d - 1]) for d in (1, 2, 3)], y_r.at[g], ys, ry)

        def stage1():
            arrived(hold["y"])
            sy[...] = src[y] + ry[0] + (ry[1] + ry[2])
            hold["z"] = sends([(sy.at[z ^ d], rz.at[d - 1]) for d in (1, 2, 3)], z_r.at[g], zs, rz)

        def stage2():
            arrived(hold["z"])
            total = sy[z] + rz[0] + (rz[1] + rz[2])
            sx[...] = total
            rx[spot2] = total
            hold["x"] = sends([(sx, rx.at[spot2])] * 3, x_r.at[g], xs2, rx.at[three])

        def stage3():
            arrived(hold["x"])
            gz[z] = rx[:2] + rx[2:]
            hold["az"] = sends([(gz.at[z], gz.at[z])] * 3, az_r.at[g], zs, gz.at[three])

        def stage4():
            arrived(hold["az"])
            hold["ay"] = sends([(gz, gy.at[core, y])] * 3, ay_r.at[g], ys, gy.at[core, three])
            gy[core, y] = gz[...]

        def stage5():
            arrived(hold["ay"])
            hold["pair"] = sends([(gy.at[core], gy.at[core])], pair_r.at[g], pair, gy.at[core])

        def stage6():
            arrived(hold["pair"])

        return stage0, stage1, stage2, stage3, stage4, stage5, stage6

    D = scattered(0, d_src, d_ry, d_sy, d_rz, d_sx, d_rx, d_gz, d_gy)
    E = scattered(1, e_src, e_ry, e_sy, e_rz, e_sx, e_rx, e_gz, e_gy)

    def f0(i):
        return sends([(f_src.at[i, y ^ d], f_ry.at[i, d - 1]) for d in (1, 2, 3)], y_r.at[2 + i], ys, f_ry.at[i])

    def f1(i, cps):
        arrived(cps)
        total = f_src[i, y] + f_ry[i, 0] + (f_ry[i, 1] + f_ry[i, 2])
        f_sy[i] = total
        f_rz[i, z] = total
        return sends([(f_sy.at[i], f_rz.at[i, z])] * 3, z_r.at[2 + i], zs, f_rz.at[i, three])

    def f2(i, cps):
        arrived(cps)
        total = (f_rz[i, 0] + f_rz[i, 1]) + (f_rz[i, 2] + f_rz[i, 3])
        f_sx[i] = total
        f_rx[i, spot2] = total
        return sends([(f_sx.at[i], f_rx.at[i, spot2])] * 3, x_r.at[2 + i], xs2, f_rx.at[i, three])

    def f3(i, cps):
        arrived(cps)
        f_gz[i] = f_rx[i, :2] + f_rx[i, 2:]
        out = sends([(f_gz.at[i], f_gy.at[i, core, y])] * 3, ay_r.at[2 + i], ys, f_gy.at[i, core, three])
        f_gy[i, core, y] = f_gz[i]
        return out

    def f4(i, cps):
        arrived(cps)
        whole = f_gy.at[i, core]
        return sends([(whole, whole)], pair_r.at[2 + i], pair, whole)

    def t0(i):
        t_ry[i, y] = t_src[i]
        return sends([(t_src.at[i], t_ry.at[i, y])] * 3, y_r.at[5 + i], ys, t_ry.at[i, three])

    def t1(i, cps):
        arrived(cps)
        total = (t_ry[i, 0] + t_ry[i, 1]) + (t_ry[i, 2] + t_ry[i, 3])
        t_sy[i] = total
        t_rz[i, z] = total
        return sends([(t_sy.at[i], t_rz.at[i, z])] * 3, z_r.at[5 + i], zs, t_rz.at[i, three])

    def t2(i, cps):
        arrived(cps)
        total = (t_rz[i, 0] + t_rz[i, 1]) + (t_rz[i, 2] + t_rz[i, 3])
        t_sx[i] = total
        t_rx[i, spot] = total
        return sends([(t_sx.at[i], t_rx.at[i, spot])] * 7, x_r.at[5 + i], xs, t_rx.at[i, seven])

    D[0]()
    split_rows(c, tt.at[mine + core])
    tq.wait_recv()
    split_rows(sib, stt)

    def chunk_part(j, k, first, count):
        w, n = columns(j), WIDTHS[j]

        def body(t, total):
            o = pl.multiple_of(first + t * 1024, 1024)
            x = rt[k, w, pl.ds(o, 1024)]
            h = x.astype(bf16).astype(f32)
            both = jnp.concatenate([h, x - h], 0).astype(bf16)
            a, b = dot(both, wh[k, pl.ds(o, 1024), :]), dot(both, wl[k, pl.ds(o, 1024), :])
            return total + (a[:n] + ((a[n:] + b[:n]) + b[n:]))

        zero = jnp.zeros((n, 256), f32)
        return body(0, zero) if count == 1 else lax.fori_loop(0, count, body, zero)

    def store_cover(r, k, x):
        for ref, part in zip((g1, g2, g3), split3(x)):
            ref[r : r + 128, k : k + 256] = part

    def issue(i):
        if i < 2 * CHUNKS:
            send_chunk(i // 2, i % 2)

    f, t = {}, {}
    for j in range(CHUNKS):
        w = columns(j)
        last = j == CHUNKS - 1
        arrived(exchange[j, 0])
        total = chunk_part(j, 0, 0, 2)
        if j == 5:
            E[2]()
        if last:
            arrived(exchange[j, 1][:1])
            total = total + chunk_part(j, 1, 0, 1)
            f[2] = f1(2, f[2])
            arrived(exchange[j, 1][1:])
            total = total + chunk_part(j, 1, 1024, 1)
        else:
            arrived(exchange[j, 1])
        if j == 2:
            D[2]()
        if j == 6:
            f[0] = f2(0, f[0])
        for k in range(2):
            issue(2 * j + 4 + k)
        if not last:
            total = total + chunk_part(j, 1, 0, 2)
        if j < 7:
            for i in range(2):
                for n in range(2):
                    unit = total[8 * i : 8 * i + 8, 128 * n : 128 * n + 128]
                    if j < 4:
                        e_src[j, 2 * i + n] = unit
                    else:
                        f_src[j - 4, 2 * i + n] = unit
            if j >= 4:
                f[j - 4] = f0(j - 4)
        else:
            t_src[j - 7] = total
            t[j - 7] = t0(j - 7)
        send_apart(rt.at[1 - core, w], frt.at[w], fw_s, fw_r, at_col(sib))
        if j < 7:
            h, l = split2(rt[core, w, :])
            ih[par, w, :] = h
            il[par, w, :] = l
        if j == 1:
            D[1]()
        if j == 3:
            E[0]()
        if j == 4:
            D[3]()
            E[1]()
        if j == 5:
            D[4]()
            f[0] = f1(0, f[0])
        if j == 6:
            f[1] = f1(1, f[1])
            D[5]()
            E[3]()
            D[6]()
            for k in range(4):
                store_cover(128 * k, 256 * (k // 2), d_gy[k % 2, :, :, k // 2].reshape(128, 256))
    f[1] = f2(1, f[1])
    E[4]()
    t[0] = t1(0, t[0])
    h, l = split2(rt[core, 112:128, :])
    ih[par, 112:128, :] = h
    il[par, 112:128, :] = l
    f[0] = f3(0, f[0])
    f[2] = f2(2, f[2])
    t[1] = t1(1, t[1])
    f[1] = f3(1, f[1])
    E[5]()
    t[0] = t2(0, t[0])
    f[0] = f4(0, f[0])
    f[2] = f3(2, f[2])
    E[6]()
    for k in range(4):
        for r in range(4):
            for i in range(2):
                for n in range(2):
                    unit = e_gy[k % 2, r, 2 * i + n, k // 2]
                    xg[k, 16 * r + 8 * i : 16 * r + 8 * i + 8, 128 * n : 128 * n + 128] = unit
    t[1] = t2(1, t[1])
    f[1] = f4(1, f[1])
    f[2] = f4(2, f[2])
    arrived(starts)
    vectors = jnp.concatenate([rst[k] for k in range(4)], 1)
    forwards = Waits(frt, fw_s, fw_r)
    pending.append(forwards)
    forwards.wait_recv()
    split_rows(dia, frt)
    for j in range(3):
        arrived(f[j])
        for k in range(4):
            for i in range(2):
                for n in range(2):
                    r = 64 + 16 * j + 8 * i
                    xg[k, r : r + 8, 128 * n : 128 * n + 128] = f_gy[j, k % 2, 2 * i + n, k // 2]
    for j in range(2):
        arrived(t[j])
        for k in range(4):
            r = 112 + 8 * j
            xg[k, r : r + 8, :] = t_rx[j, k] + t_rx[j, 4 + k]
    across, below = xg[2:4].reshape(256, 256), xg[0:2].reshape(256, 256)
    upper, below = across + below.T, below + across.T
    store_cover(0, 256, upper[:128])
    store_cover(128, 256, upper[128:])
    store_cover(256, 0, below[:128])
    store_cover(384, 0, below[128:])

    def step(vectors):
        products = times_cover(vectors, g1, g2, g3)
        return orthonormal(outer_gram(products), products)

    vectors = lax.fori_loop(0, STEPS - 1, lambda i, v: step(v)[0], vectors)

    vh, vl = split2(vectors)
    vb = jnp.concatenate([vh, vl], 0)
    images = []
    for n in range(PIECES):
        o = pl.ds(IW * n, IW)
        h = jnp.concatenate([ih[k, :, o] for k in range(4)], 0)
        l = jnp.concatenate([il[k, :, o] for k in range(4)], 0)
        both = dot(vb, h)
        part = both[:16] + (both[16:] + dot(vh, l))
        img[n] = part
        limg[n, c] = part
        images.append(send_apart(img.at[n], limg.at[n, c], im_s.at[0], im_r.at[n], at_col(par)))
        send_apart(img.at[n], limg.at[n, c], im_s.at[1], im_r.at[PIECES], at_col(sib))
        if n == PIECES - 1:
            direct = send_apart(img.at[n], limg.at[n, c], im_s.at[2], im_r.at[PIECES + 1], at_col(dia))
    vectors, diagonal = step(vectors)
    for k in range(4):
        vs[k] = vectors[:, 128 * k : 128 * k + 128]
    right_o[...] = vs[c]
    eye = lax.broadcasted_iota(jnp.int32, (16, 128), 0) == lax.broadcasted_iota(jnp.int32, (16, 128), 1)
    str_o[...] = jnp.sum(jnp.where(eye, diagonal / rows_total, 0.0), 0, keepdims=True)[:, :16]

    for n in range(PIECES):
        images[n].wait_recv()
        if n < PIECES - 1:
            send_apart(limg.at[n, par], limg.at[n, par], if_s, if_r, at_col(sib))
    local, relays = Waits(img, im_s.at[1], im_r.at[PIECES]), Waits(img.at[: PIECES - 1], if_s, if_r)
    local.wait_recv()
    direct.wait_recv()
    relays.wait_recv()
    for n in range(PIECES):
        for k in range(4):
            left_o[:, 2048 * k + IW * n : 2048 * k + IW * n + IW] = limg[n, k]
    pending += [local, relays, direct, Waits(img, im_s.at[0], im_s.at[0])]
    pending.append(Waits(tab.at[0, :2], ex_s, ex_s))
    pending.append(Waits(tab.at[0, :4, pl.ds(0, 2 * sent[0])], all_s, all_s))
    for cp in pending:
        cp.wait_send()


def write_out(a, b, d, ao, bo, do, sem):
    copies = [pltpu.make_async_copy(x, o, sem.at[i]) for i, (x, o) in enumerate(((a, ao), (b, bo), (d, do)))]
    for cp in copies:
        cp.start()
    for cp in copies:
        cp.wait()


def scattered_scratch(*unit):
    V = pltpu.VMEM
    return [
        V((4, 4, *unit), f32),
        V((3, 4, *unit), f32),
        V((4, *unit), f32),
        V((3, *unit), f32),
        V(unit, f32),
        V((4, *unit), f32),
        V((4, 2, *unit), f32),
        V((2, 4, 4, 2, *unit), f32),
    ]


def on_device(rows_total, table, start):
    V, D = pltpu.VMEM, pltpu.SemaphoreType.DMA
    scratch = [
        V((2, 4, 2048, 128), f32),
        V((4, 128, 2048), f32),
        V((2, 128, 2048), f32),
        V((128, 2048), f32),
        V((128, 2048), f32),
        V((2, 2048, 256), bf16),
        V((2, 2048, 256), bf16),
        V((4, 128, 2048), bf16),
        V((4, 128, 2048), bf16),
        V((4, 16, 128), f32),
        *scattered_scratch(8, 256),
        *scattered_scratch(8, 128),
        V((3, 4, 8, 128), f32),
        V((3, 3, 8, 128), f32),
        V((3, 8, 128), f32),
        V((3, 4, 8, 128), f32),
        V((3, 8, 128), f32),
        V((3, 4, 8, 128), f32),
        V((3, 2, 8, 128), f32),
        V((3, 2, 4, 2, 8, 128), f32),
        V((2, 8, 256), f32),
        V((2, 4, 8, 256), f32),
        V((2, 8, 256), f32),
        V((2, 4, 8, 256), f32),
        V((2, 8, 256), f32),
        V((2, 8, 8, 256), f32),
        V((4, 128, 256), f32),
        V((512, 512), bf16),
        V((512, 512), bf16),
        V((512, 512), bf16),
        V((PIECES, 16, IW), f32),
        V((PIECES, 4, 16, IW), f32),
        V((4, 16, 128), f32),
        D((7,)),
        D, D,
        D, D((4,)),
        D, D,
        D, D((CHUNKS + 1, 2)),
        D, D,
        D,
        D((7,)), D((7,)), D((7,)),
        D((2,)), D((5,)), D((5,)),
        D((3,)), D((PIECES + 2,)),
        D, D,
    ]
    table, start = (pltpu.with_memory_space_constraint(x, pltpu.HBM) for x in (table, start))
    results = pl.pallas_call(
        functools.partial(kernel, rows_total),
        out_shape=[V((16, 128), f32), V((16, 8192), f32), V((1, 16), f32)],
        in_specs=[pl.BlockSpec(memory_space=pltpu.HBM)] * 2,
        out_specs=[pl.BlockSpec(memory_space=V)] * 3,
        scratch_shapes=scratch,
        compiler_params=pltpu.CompilerParams(
            collective_id=0, has_side_effects=True, vmem_limit_bytes=48 * 1024 * 1024
        ),
    )(table, start)
    right, left, strengths = pl.pallas_call(
        write_out,
        out_shape=[jax.ShapeDtypeStruct(x.shape, f32) for x in results],
        in_specs=[pl.BlockSpec(memory_space=V)] * 3,
        out_specs=[pl.BlockSpec(memory_space=pl.ANY)] * 3,
        scratch_shapes=[D((3,))],
        compiler_params=pltpu.CompilerParams(vmem_limit_bytes=1024 * 1024),
    )(*results)
    return right, left, strengths.reshape(16)


def solution(mesh):
    rows_total = 8192 * mesh.shape["rowa"] * mesh.shape["rowb"]
    return jax.shard_map(
        functools.partial(on_device, rows_total),
        mesh=mesh,
        in_specs=(P(("rowa", "rowb"), "col"), P(None, "col")),
        out_specs=(P(None, "col"), P(None, ("rowa", "rowb")), P()),
        check_vma=False,
    )
```

```python
import functools
import math

import jax
import jax.numpy as jnp
from jax import lax
from jax.experimental import pallas as pl
from jax.experimental.pallas import tpu as pltpu
from jax.sharding import PartitionSpec as P

STEPS = 8
MESH = pl.DeviceIdType.MESH
f32 = jnp.float32
bf16 = jnp.bfloat16
WIDTHS = (16, 16, 16, 16, 16, 16, 16, 8, 8)
CHUNKS = len(WIDTHS)
LAST = (((0, 0, 2048),), ((1, 0, 1024), (2, 1024, 1024)))
PIECES = 8
IW = 2048 // PIECES


def dot(a, b):
    return lax.dot_general(a, b, (((1,), (0,)), ((), ())), preferred_element_type=f32)


def dot_nt(a, b):
    return lax.dot_general(a, b, (((1,), (1,)), ((), ())), preferred_element_type=f32)


def split2(x):
    h = x.astype(bf16)
    return h, (x - h.astype(f32)).astype(bf16)


def split3(x):
    h = x.astype(bf16)
    r = x - h.astype(f32)
    m = r.astype(bf16)
    return h, m, (r - m.astype(f32)).astype(bf16)


def times_cover(v, g1, g2, g3):
    h, m, l = split3(v)
    a = jnp.concatenate([h, m, l], 0)
    o1, o2, o3 = dot(a, g1[...]), dot(a[:32], g2[...]), dot(h, g3[...])
    return o1[:16] + (o1[16:32] + o2[:16]) + (o1[32:] + o2[16:] + o3)


def outer_gram(p):
    h, m, l = split3(p)
    a = jnp.concatenate([h, m, l], 0)
    o1, o2, o3 = dot_nt(a, h), dot_nt(a[:32], m), dot_nt(h, l)
    return o1[:16] + (o1[16:32] + o2[:16]) + (o1[32:] + o2[16:] + o3)


def orthonormal(gram, p):
    rows = lax.broadcasted_iota(jnp.int32, (16, 128), 0)
    cols = [jnp.broadcast_to(gram[:, k : k + 1], (16, 128)) for k in range(16)]
    tiles = [p[:, 128 * t : 128 * t + 128] for t in range(4)]
    pivots = jnp.zeros((16, 128), f32)
    for k in range(16):
        d = cols[k][k : k + 1, :]
        pivots = jnp.where(rows == k, d, pivots)
        if k < 15:
            m = jnp.where(rows > k, cols[k] * (1.0 / d), 0.0)
            for j in range(k + 1, 16):
                cols[j] = cols[j] - m * cols[j][k : k + 1, :]
            tiles = [t - m * t[k : k + 1, :] for t in tiles]
    s = jnp.sqrt(pivots)
    r = 1.0 / s
    return jnp.concatenate([t * r for t in tiles], 1), s


def kernel(
    rows_total,
    table, start, right_o, left_o, str_o,
    tab, tt, rt, stt, frt, r8, wh, wl, ih, il, rst,
    d_src, d_ry, d_sy, d_rz, d_sx, d_rx, d_gz, d_gy,
    e_src, e_ry, e_sy, e_rz, e_sx, e_rx, e_gz, e_gy,
    f_src, f_ry, f_sy, f_rz, f_sx, f_rx, f_gz, f_gy,
    t_src, t_ry, t_sy, t_rz, t_sx, t_rx,
    u_src, u_ry, u_sy, u_rz, u_sx, u_rx,
    c_src, c_ry, c_sy, c_rz, c_sx, c_rx, xg,
    g1, g2, g3, img, limg, vs,
    load_s, st_l, st_r, nat_s, nat_r, tq_s, tq_r, ex_s, ex_r, fw_s, fw_r,
    all_s, y_r, z_r, x_r, az_r, ay_r, pair_r, r8_r, c_s, c_r, r8f_s, r8f_r,
    im_s, im_r, if_s, if_r,
):
    ra, rb, c = lax.axis_index("rowa"), lax.axis_index("rowb"), lax.axis_index("col")
    y, z = rb % 4, rb // 4
    core, half = c % 2, c // 2
    mine, other = 2 * half, 2 - 2 * half
    sib, par, dia = c ^ 1, c ^ 2, c ^ 3

    def at_col(k):
        return (ra, rb, k)

    def at_y(d):
        return (ra, z * 4 + (y ^ d), c)

    def at_z(d):
        return (ra, (z ^ d) * 4 + y, c)

    def at_x(da, dc):
        return (ra ^ da, rb, c ^ dc)

    pending = []

    def send(a, b, s, r, dev):
        cp = pltpu.make_async_remote_copy(
            src_ref=a, dst_ref=b, send_sem=s, recv_sem=r, device_id=dev, device_id_type=MESH
        )
        cp.start()
        pending.append(cp)
        return cp

    def send_apart(*args):
        cp = send(*args)
        pending.pop()
        return cp

    class Waits:
        def __init__(self, whole, s, r):
            self.whole, self.s, self.r = whole, s, r

        def wait_send(self):
            pltpu.make_async_copy(self.whole, self.whole, self.s).wait()

        def wait_recv(self):
            pltpu.make_async_copy(self.whole, self.whole, self.r).wait()

    sent = [0]

    def sends(pairs, r, devs, whole):
        for (a, b), dev in zip(pairs, devs, strict=True):
            send_apart(a, b, all_s, r, dev)
        sent[0] += math.prod(whole.shape) // 1024
        return [Waits(whole, all_s, r)]

    three, seven = pl.ds(0, 3), pl.ds(0, 7)
    spot, spot2 = ra * 4 + c, ra * 2 + half
    pair = [at_col(sib)]

    def arrived(copies):
        for cp in copies:
            cp.wait_recv()

    XP = [(da, dc) for da in range(2) for dc in range(4) if (da, dc) != (0, 0)]

    own_start = pltpu.make_async_copy(start, rst.at[c], st_l)

    def load(i, q, o, n):
        cp = pltpu.make_async_copy(
            table.at[pl.ds(q * 2048 + o, n), :], tab.at[core, q, pl.ds(o, n), :], load_s.at[i]
        )
        cp.start()
        return cp

    loads = [load(p, other, 512 * p, 512) for p in range(4)]
    loads += [load(4 + i, q, 0, 2048) for i, q in enumerate((other + 1, mine, mine + 1))]
    own_start.start()

    barrier = pltpu.get_barrier_semaphore()
    for d in (1, 2, 3):
        pl.semaphore_signal(barrier, inc=1, device_id=at_y(d), device_id_type=MESH)
        pl.semaphore_signal(barrier, inc=1, device_id=at_z(d), device_id_type=MESH)
    for da, dc in XP:
        pl.semaphore_signal(barrier, inc=1, device_id=at_x(da, dc), device_id_type=MESH)

    def transpose_rows(q, first, blocks):
        def body(i, carry):
            o = pl.multiple_of(first + i * 256, 256)
            tt[q, :, pl.ds(o, 256)] = tab[core, q, pl.ds(o, 256), :].T
            return carry

        lax.fori_loop(0, blocks, body, 0)

    def columns(j):
        return pl.ds(sum(WIDTHS[:j]), WIDTHS[j])

    exchange = {}

    def send_chunk(j, k):
        w = columns(j)
        if j == CHUNKS - 1:
            for i, o, n in LAST[k]:
                part = pl.ds(o, n)
                send_apart(tt.at[other + k, w, part], r8.at[core, k, :, part], ex_s, r8_r.at[core, i], at_col(3 - 2 * half))
            return
        exchange[j, k] = [send_apart(tt.at[other + k, w], rt.at[k, w], ex_s, ex_r.at[j, k], at_col(par))]

    for p in range(4):
        loads[p].wait()
        transpose_rows(other, 512 * p, 2)
        if p == 0:
            pl.semaphore_wait(barrier, 13)
        o = pl.ds(512 * p, 512)
        send_apart(tt.at[other, columns(0), o], rt.at[0, columns(0), o], ex_s, ex_r.at[0, 0], at_col(par))
    whole = rt.at[0, columns(0)]
    exchange[0, 0] = [Waits(whole, ex_s, ex_r.at[0, 0])]
    nat = []
    for i, q in enumerate((mine, mine + 1, other, other + 1)):
        nat.append(
            send_apart(table.at[pl.ds(q * 2048, 2048), :], tab.at[core, q], nat_s, nat_r.at[i], at_col(sib))
        )
    pending.append(Waits(tab.at[0], nat_s, nat_s))
    loads[4].wait()
    transpose_rows(other + 1, 0, 8)
    for j, k in ((0, 1), (1, 0), (1, 1)):
        send_chunk(j, k)
    own_start.wait()
    starts = sends([(rst.at[c], rst.at[c])] * 3, st_r, [at_col(c ^ d) for d in (1, 2, 3)], rst.at[three])
    loads[5].wait()
    transpose_rows(mine, 0, 8)
    loads[6].wait()
    transpose_rows(mine + 1, 0, 8)
    tq = send(tt.at[mine + 1 - core], stt, tq_s, tq_r, at_col(sib))

    acc = jnp.zeros((128, 256), f32)
    for i, q in enumerate((mine, mine + 1, other, other + 1)):
        nat[i].wait_recv()

        def body(t, acc, i=i, q=q):
            o = pl.multiple_of(t * 512, 512)
            w = jnp.concatenate([tab[0, q, pl.ds(o, 512), :], tab[1, q, pl.ds(o, 512), :]], 1)
            h, l = split2(w)
            if i < 2:
                wh[i, pl.ds(o, 512), :] = h
                wl[i, pl.ds(o, 512), :] = l
            ah, al = split2(tt[q, :, pl.ds(o, 512)])
            both = dot(jnp.concatenate([ah, al], 0), h)
            return acc + (both[:128] + (both[128:] + dot(ah, l)))

        acc = lax.fori_loop(0, 4, body, acc)
    d_src[...] = acc.reshape(4, 4, 8, 256)

    def split_rows(block, ref):
        def body(i, carry):
            o = pl.multiple_of(i * 512, 512)
            h, l = split2(ref[:, pl.ds(o, 512)])
            ih[block, :, pl.ds(o, 512)] = h
            il[block, :, pl.ds(o, 512)] = l
            return carry

        lax.fori_loop(0, 4, body, 0)

    ys, zs = [at_y(d) for d in (1, 2, 3)], [at_z(d) for d in (1, 2, 3)]
    xs = [at_x(da, dc) for da, dc in XP]
    xs2 = [at_x(da, dc) for da, dc in ((0, 2), (1, 0), (1, 2))]

    def scattered(g, src, ry, sy, rz, sx, rx, gz, gy):
        hold = {}

        def stage0():
            hold["y"] = sends([(src.at[y ^ d], ry.at[d - 1]) for d in (1, 2, 3)], y_r.at[g], ys, ry)

        def stage1():
            arrived(hold["y"])
            sy[...] = src[y] + ry[0] + (ry[1] + ry[2])
            hold["z"] = sends([(sy.at[z ^ d], rz.at[d - 1]) for d in (1, 2, 3)], z_r.at[g], zs, rz)

        def stage2():
            arrived(hold["z"])
            total = sy[z] + rz[0] + (rz[1] + rz[2])
            sx[...] = total
            rx[spot2] = total
            hold["x"] = sends([(sx, rx.at[spot2])] * 3, x_r.at[g], xs2, rx.at[three])

        def stage3():
            arrived(hold["x"])
            gz[z] = rx[:2] + rx[2:]
            hold["az"] = sends([(gz.at[z], gz.at[z])] * 3, az_r.at[g], zs, gz.at[three])

        def stage4():
            arrived(hold["az"])
            hold["ay"] = sends([(gz, gy.at[core, y])] * 3, ay_r.at[g], ys, gy.at[core, three])
            gy[core, y] = gz[...]

        def stage5():
            arrived(hold["ay"])
            hold["pair"] = sends([(gy.at[core], gy.at[core])], pair_r.at[g], pair, gy.at[core])

        def stage6():
            arrived(hold["pair"])

        return stage0, stage1, stage2, stage3, stage4, stage5, stage6

    D = scattered(0, d_src, d_ry, d_sy, d_rz, d_sx, d_rx, d_gz, d_gy)
    E = scattered(1, e_src, e_ry, e_sy, e_rz, e_sx, e_rx, e_gz, e_gy)

    def f0(i):
        return sends([(f_src.at[i, y ^ d], f_ry.at[i, d - 1]) for d in (1, 2, 3)], y_r.at[2 + i], ys, f_ry.at[i])

    def f1(i, cps):
        arrived(cps)
        total = f_src[i, y] + f_ry[i, 0] + (f_ry[i, 1] + f_ry[i, 2])
        f_sy[i] = total
        f_rz[i, z] = total
        return sends([(f_sy.at[i], f_rz.at[i, z])] * 3, z_r.at[2 + i], zs, f_rz.at[i, three])

    def f2(i, cps):
        arrived(cps)
        total = (f_rz[i, 0] + f_rz[i, 1]) + (f_rz[i, 2] + f_rz[i, 3])
        f_sx[i] = total
        f_rx[i, spot2] = total
        return sends([(f_sx.at[i], f_rx.at[i, spot2])] * 3, x_r.at[2 + i], xs2, f_rx.at[i, three])

    def f3(i, cps):
        arrived(cps)
        f_gz[i] = f_rx[i, :2] + f_rx[i, 2:]
        out = sends([(f_gz.at[i], f_gy.at[i, core, y])] * 3, ay_r.at[2 + i], ys, f_gy.at[i, core, three])
        f_gy[i, core, y] = f_gz[i]
        return out

    def f4(i, cps):
        arrived(cps)
        whole = f_gy.at[i, core]
        return sends([(whole, whole)], pair_r.at[2 + i], pair, whole)

    T = (
        (t_src, t_ry, t_sy, t_rz, t_sx, t_rx),
        (u_src, u_ry, u_sy, u_rz, u_sx, u_rx),
    )

    def t0(i):
        src, ry = T[i][:2]
        ry[y] = src[...]
        return sends([(src, ry.at[y])] * 3, y_r.at[4 + i], ys, ry.at[three])

    def t1(i, cps):
        ry, sy, rz = T[i][1:4]
        arrived(cps)
        total = (ry[0] + ry[1]) + (ry[2] + ry[3])
        sy[...] = total
        rz[z] = total
        return sends([(sy, rz.at[z])] * 3, z_r.at[4 + i], zs, rz.at[three])

    def t2(i, cps):
        rz, sx, rx = T[i][3:]
        arrived(cps)
        total = (rz[0] + rz[1]) + (rz[2] + rz[3])
        sx[...] = total
        rx[spot] = total
        return sends([(sx, rx.at[spot])] * 7, x_r.at[4 + i], xs, rx.at[seven])

    def on_core_1(stage):
        pl.when(core == 1)(stage)

    def c_send(a, b, i, devs):
        for dev in devs:
            send_apart(a, b, c_s, c_r.at[i], dev)

    def last_part(k, o, total):
        x = r8[:, k, :, pl.ds(o, 1024)].reshape(16, 1024)
        h = x.astype(bf16).astype(f32)
        both = jnp.concatenate([h, x - h], 0).astype(bf16)
        a, b = dot(both, wh[k, pl.ds(o, 1024), :]), dot(both, wl[k, pl.ds(o, 1024), :])
        return total + (a[:16] + ((a[16:] + b[:16]) + b[16:]))

    def c0():
        total = jnp.zeros((16, 256), f32)
        for k in range(2):
            for i, o, n in LAST[k]:
                for q in range(2):
                    Waits(r8.at[q, k, :, pl.ds(o, n)], ex_s, r8_r.at[q, i]).wait_recv()
                for first in range(o, o + n, 1024):
                    total = last_part(k, first, total)
        c_src[...] = total
        c_ry[y] = total
        c_send(c_src, c_ry.at[y], 0, ys)
        send_apart(r8.at[:, 0], r8.at[:, 0], r8f_s, r8f_r, at_col(sib))

    def c1():
        Waits(c_ry.at[three], c_s, c_r.at[0]).wait_recv()
        total = (c_ry[0] + c_ry[1]) + (c_ry[2] + c_ry[3])
        c_sy[...] = total
        c_rz[z] = total
        c_send(c_sy, c_rz.at[z], 1, zs)

    def c2():
        Waits(c_rz.at[three], c_s, c_r.at[1]).wait_recv()
        total = (c_rz[0] + c_rz[1]) + (c_rz[2] + c_rz[3])
        c_sx[...] = total
        c_rx[spot2] = total
        c_send(c_sx, c_rx.at[spot2], 2, xs)

    D[0]()
    split_rows(c, tt.at[mine + core])
    tq.wait_recv()
    split_rows(sib, stt)

    def chunk_part(j, k, first, count):
        w, n = columns(j), WIDTHS[j]

        def body(t, total):
            o = pl.multiple_of(first + t * 1024, 1024)
            x = rt[k, w, pl.ds(o, 1024)]
            h = x.astype(bf16).astype(f32)
            both = jnp.concatenate([h, x - h], 0).astype(bf16)
            a, b = dot(both, wh[k, pl.ds(o, 1024), :]), dot(both, wl[k, pl.ds(o, 1024), :])
            return total + (a[:n] + ((a[n:] + b[:n]) + b[n:]))

        zero = jnp.zeros((n, 256), f32)
        return body(0, zero) if count == 1 else lax.fori_loop(0, count, body, zero)

    def store_cover(r, k, x):
        for ref, part in zip((g1, g2, g3), split3(x)):
            ref[r : r + 128, k : k + 256] = part

    def issue(i):
        if i < 2 * CHUNKS:
            send_chunk(i // 2, i % 2)

    f, t = {}, {}
    for j in range(CHUNKS):
        w = columns(j)
        last = j == CHUNKS - 1
        if last:
            on_core_1(c0)
            break
        arrived(exchange[j, 0])
        total = chunk_part(j, 0, 0, 2)
        if j == 5:
            E[2]()
        arrived(exchange[j, 1])
        if j == 2:
            D[2]()
        if j == 6:
            f[0] = f2(0, f[0])
        for k in range(2):
            issue(2 * j + 4 + k)
        total = total + chunk_part(j, 1, 0, 2)
        if j < 6:
            for i in range(2):
                for n in range(2):
                    unit = total[8 * i : 8 * i + 8, 128 * n : 128 * n + 128]
                    if j < 4:
                        e_src[j, 2 * i + n] = unit
                    else:
                        f_src[j - 4, 2 * i + n] = unit
            if j >= 4:
                f[j - 4] = f0(j - 4)
        else:
            T[j - 6][0][...] = total
            t[j - 6] = t0(j - 6)
        send_apart(rt.at[1 - core, w], frt.at[w], fw_s, fw_r, at_col(sib))
        if j < 7:
            h, l = split2(rt[core, w, :])
            ih[par, w, :] = h
            il[par, w, :] = l
        if j == 1:
            D[1]()
        if j == 3:
            E[0]()
        if j == 4:
            D[3]()
            E[1]()
        if j == 5:
            D[4]()
            f[0] = f1(0, f[0])
        if j == 6:
            f[1] = f1(1, f[1])
            D[5]()
            E[3]()
            D[6]()
            for k in range(4):
                store_cover(128 * k, 256 * (k // 2), d_gy[k % 2, :, :, k // 2].reshape(128, 256))
    t[0] = t1(0, t[0])
    f[1] = f2(1, f[1])
    t[1] = t1(1, t[1])
    on_core_1(c1)
    t[0] = t2(0, t[0])
    E[4]()
    f[0] = f3(0, f[0])
    f[1] = f3(1, f[1])
    t[1] = t2(1, t[1])
    on_core_1(c2)
    E[5]()
    f[0] = f4(0, f[0])
    f[1] = f4(1, f[1])
    forwards = Waits(frt.at[:120], fw_s, fw_r)
    pending.append(forwards)
    forwards.wait_recv()
    to_core_0 = Waits(r8.at[:, 0], r8f_s, r8f_r)
    pl.when(core == 0)(to_core_0.wait_recv)
    frt[120:128, :] = r8[1 - core, core]
    rt[core, 120:128, :] = r8[core, core]
    split_rows(dia, frt)
    h, l = split2(rt[core, 112:128, :])
    ih[par, 112:128, :] = h
    il[par, 112:128, :] = l
    E[6]()
    for k in range(4):
        for r in range(4):
            for i in range(2):
                for n in range(2):
                    unit = e_gy[k % 2, r, 2 * i + n, k // 2]
                    xg[k, 16 * r + 8 * i : 16 * r + 8 * i + 8, 128 * n : 128 * n + 128] = unit
    arrived(starts)
    vectors = jnp.concatenate([rst[k] for k in range(4)], 1)
    for j in range(2):
        arrived(f[j])
        for k in range(4):
            for i in range(2):
                for n in range(2):
                    r = 64 + 16 * j + 8 * i
                    xg[k, r : r + 8, 128 * n : 128 * n + 128] = f_gy[j, k % 2, 2 * i + n, k // 2]
    for j in range(2):
        arrived(t[j])
        rx = T[j][5]
        for k in range(4):
            xg[k, columns(6 + j), :] = rx[k] + rx[4 + k]
    on_core_1(Waits(c_rx.at[three], c_s, c_r.at[2]).wait_recv)
    pl.when(core == 0)(Waits(c_rx, c_s, c_r.at[2]).wait_recv)
    for k in range(4):
        i = pl.ds(8 * (k % 2), 8)
        xg[k, 120:128, :] = c_rx[k // 2, i] + c_rx[2 + k // 2, i]
    across, below = xg[2:4].reshape(256, 256), xg[0:2].reshape(256, 256)
    upper, below = across + below.T, below + across.T
    store_cover(0, 256, upper[:128])
    store_cover(128, 256, upper[128:])
    store_cover(256, 0, below[:128])
    store_cover(384, 0, below[128:])

    def step(vectors):
        products = times_cover(vectors, g1, g2, g3)
        return orthonormal(outer_gram(products), products)

    vectors = lax.fori_loop(0, STEPS - 1, lambda i, v: step(v)[0], vectors)

    vh, vl = split2(vectors)
    vb = jnp.concatenate([vh, vl], 0)
    images = []
    for n in range(PIECES):
        o = pl.ds(IW * n, IW)
        h = jnp.concatenate([ih[k, :, o] for k in range(4)], 0)
        l = jnp.concatenate([il[k, :, o] for k in range(4)], 0)
        both = dot(vb, h)
        part = both[:16] + (both[16:] + dot(vh, l))
        img[n] = part
        limg[n, c] = part
        images.append(send_apart(img.at[n], limg.at[n, c], im_s.at[0], im_r.at[n], at_col(par)))
        send_apart(img.at[n], limg.at[n, c], im_s.at[1], im_r.at[PIECES], at_col(sib))
        if n == PIECES - 1:
            direct = send_apart(img.at[n], limg.at[n, c], im_s.at[2], im_r.at[PIECES + 1], at_col(dia))
    vectors, diagonal = step(vectors)
    for k in range(4):
        vs[k] = vectors[:, 128 * k : 128 * k + 128]
    right_o[...] = vs[c]
    eye = lax.broadcasted_iota(jnp.int32, (16, 128), 0) == lax.broadcasted_iota(jnp.int32, (16, 128), 1)
    str_o[...] = jnp.sum(jnp.where(eye, diagonal / rows_total, 0.0), 0, keepdims=True)[:, :16]

    for n in range(PIECES):
        images[n].wait_recv()
        if n < PIECES - 1:
            send_apart(limg.at[n, par], limg.at[n, par], if_s, if_r, at_col(sib))
    local, relays = Waits(img, im_s.at[1], im_r.at[PIECES]), Waits(img.at[: PIECES - 1], if_s, if_r)
    local.wait_recv()
    direct.wait_recv()
    relays.wait_recv()
    for n in range(PIECES):
        for k in range(4):
            left_o[:, 2048 * k + IW * n : 2048 * k + IW * n + IW] = limg[n, k]
    pending += [local, relays, direct, Waits(img, im_s.at[0], im_s.at[0])]
    pending.append(Waits(tab.at[0, :2], ex_s, ex_s))
    on_core_1(Waits(tab.at[0, :4, pl.ds(0, 2 * 52)], c_s, c_s).wait_send)
    on_core_1(to_core_0.wait_send)
    pending.append(Waits(tab.at[0, :4, pl.ds(0, 2 * sent[0])], all_s, all_s))
    for cp in pending:
        cp.wait_send()


def write_out(a, b, d, ao, bo, do, sem):
    copies = [pltpu.make_async_copy(x, o, sem.at[i]) for i, (x, o) in enumerate(((a, ao), (b, bo), (d, do)))]
    for cp in copies:
        cp.start()
    for cp in copies:
        cp.wait()


def scattered_scratch(*unit):
    V = pltpu.VMEM
    return [
        V((4, 4, *unit), f32),
        V((3, 4, *unit), f32),
        V((4, *unit), f32),
        V((3, *unit), f32),
        V(unit, f32),
        V((4, *unit), f32),
        V((4, 2, *unit), f32),
        V((2, 4, 4, 2, *unit), f32),
    ]


def on_device(rows_total, table, start):
    V, D = pltpu.VMEM, pltpu.SemaphoreType.DMA
    scratch = [
        V((2, 4, 2048, 128), f32),
        V((4, 128, 2048), f32),
        V((2, 128, 2048), f32),
        V((128, 2048), f32),
        V((128, 2048), f32),
        V((2, 2, 8, 2048), f32),
        V((2, 2048, 256), bf16),
        V((2, 2048, 256), bf16),
        V((4, 128, 2048), bf16),
        V((4, 128, 2048), bf16),
        V((4, 16, 128), f32),
        *scattered_scratch(8, 256),
        *scattered_scratch(8, 128),
        V((2, 4, 8, 128), f32),
        V((2, 3, 8, 128), f32),
        V((2, 8, 128), f32),
        V((2, 4, 8, 128), f32),
        V((2, 8, 128), f32),
        V((2, 4, 8, 128), f32),
        V((2, 2, 8, 128), f32),
        V((2, 2, 4, 2, 8, 128), f32),
        V((16, 256), f32),
        V((4, 16, 256), f32),
        V((16, 256), f32),
        V((4, 16, 256), f32),
        V((16, 256), f32),
        V((8, 16, 256), f32),
        V((8, 256), f32),
        V((4, 8, 256), f32),
        V((8, 256), f32),
        V((4, 8, 256), f32),
        V((8, 256), f32),
        V((8, 8, 256), f32),
        V((16, 256), f32),
        V((4, 16, 256), f32),
        V((16, 256), f32),
        V((4, 16, 256), f32),
        V((16, 256), f32),
        V((4, 16, 256), f32),
        V((4, 128, 256), f32),
        V((512, 512), bf16),
        V((512, 512), bf16),
        V((512, 512), bf16),
        V((PIECES, 16, IW), f32),
        V((PIECES, 4, 16, IW), f32),
        V((4, 16, 128), f32),
        D((7,)),
        D, D,
        D, D((4,)),
        D, D,
        D, D((CHUNKS - 1, 2)),
        D, D,
        D,
        D((6,)), D((6,)), D((6,)),
        D((2,)), D((4,)), D((4,)),
        D((2, 3)), D, D((3,)), D, D,
        D((3,)), D((PIECES + 2,)),
        D, D,
    ]
    table, start = (pltpu.with_memory_space_constraint(x, pltpu.HBM) for x in (table, start))
    results = pl.pallas_call(
        functools.partial(kernel, rows_total),
        out_shape=[V((16, 128), f32), V((16, 8192), f32), V((1, 16), f32)],
        in_specs=[pl.BlockSpec(memory_space=pltpu.HBM)] * 2,
        out_specs=[pl.BlockSpec(memory_space=V)] * 3,
        scratch_shapes=scratch,
        compiler_params=pltpu.CompilerParams(
            collective_id=0, has_side_effects=True, vmem_limit_bytes=48 * 1024 * 1024
        ),
    )(table, start)
    right, left, strengths = pl.pallas_call(
        write_out,
        out_shape=[jax.ShapeDtypeStruct(x.shape, f32) for x in results],
        in_specs=[pl.BlockSpec(memory_space=V)] * 3,
        out_specs=[pl.BlockSpec(memory_space=pl.ANY)] * 3,
        scratch_shapes=[D((3,))],
        compiler_params=pltpu.CompilerParams(vmem_limit_bytes=1024 * 1024),
    )(*results)
    return right, left, strengths.reshape(16)


def solution(mesh):
    rows_total = 8192 * mesh.shape["rowa"] * mesh.shape["rowb"]
    return jax.shard_map(
        functools.partial(on_device, rows_total),
        mesh=mesh,
        in_specs=(P(("rowa", "rowb"), "col"), P(None, "col")),
        out_specs=(P(None, "col"), P(None, ("rowa", "rowb")), P()),
        check_vma=False,
    )
```

```python
import functools
import math

import jax
import jax.numpy as jnp
from jax import lax
from jax.experimental import pallas as pl
from jax.experimental.pallas import tpu as pltpu
from jax.sharding import PartitionSpec as P

STEPS = 8
MESH = pl.DeviceIdType.MESH
f32 = jnp.float32
bf16 = jnp.bfloat16
WIDTHS = (16, 16, 16, 16, 16, 16, 16, 8, 8)
CHUNKS = len(WIDTHS)
LAST = (((0, 0, 2048),), ((1, 0, 1024), (2, 1024, 1024)))
PIECES = 8
IW = 2048 // PIECES


def dot(a, b):
    return lax.dot_general(a, b, (((1,), (0,)), ((), ())), preferred_element_type=f32)


def dot_nt(a, b):
    return lax.dot_general(a, b, (((1,), (1,)), ((), ())), preferred_element_type=f32)


def split2(x):
    h = x.astype(bf16)
    return h, (x - h.astype(f32)).astype(bf16)


def split3(x):
    h = x.astype(bf16)
    r = x - h.astype(f32)
    m = r.astype(bf16)
    return h, m, (r - m.astype(f32)).astype(bf16)


def times_cover(v, g1, g2, g3):
    h, m, l = split3(v)
    a = jnp.concatenate([h, m, l], 0)
    o1, o2, o3 = dot(a, g1[...]), dot(a[:32], g2[...]), dot(h, g3[...])
    return o1[:16] + (o1[16:32] + o2[:16]) + (o1[32:] + o2[16:] + o3)


def outer_gram(p):
    h, m, l = split3(p)
    a = jnp.concatenate([h, m, l], 0)
    o1, o2, o3 = dot_nt(a, h), dot_nt(a[:32], m), dot_nt(h, l)
    return o1[:16] + (o1[16:32] + o2[:16]) + (o1[32:] + o2[16:] + o3)


def orthonormal(gram, p):
    rows = lax.broadcasted_iota(jnp.int32, (16, 128), 0)
    cols = [jnp.broadcast_to(gram[:, k : k + 1], (16, 128)) for k in range(16)]
    tiles = [p[:, 128 * t : 128 * t + 128] for t in range(4)]
    pivots = jnp.zeros((16, 128), f32)
    for k in range(16):
        d = cols[k][k : k + 1, :]
        pivots = jnp.where(rows == k, d, pivots)
        if k < 15:
            m = jnp.where(rows > k, cols[k] * (1.0 / d), 0.0)
            for j in range(k + 1, 16):
                cols[j] = cols[j] - m * cols[j][k : k + 1, :]
            tiles = [t - m * t[k : k + 1, :] for t in tiles]
    s = jnp.sqrt(pivots)
    r = 1.0 / s
    return jnp.concatenate([t * r for t in tiles], 1), s


def kernel(
    rows_total,
    table, start, right_o, left_o, str_o,
    tab, tt, rt, stt, frt, r8, wh, wl, ih, il, rst,
    d_src, d_ry, d_sy, d_rz, d_sx, d_rx, d_gz, d_gy,
    e_src, e_ry, e_sy, e_rz, e_sx, e_rx, e_gz, e_gy,
    f_src, f_ry, f_sy, f_rz, f_sx, f_rx, f_gz, f_gy,
    t_src, t_ry, t_sy, t_rz, t_sx, t_rx, t_gy,
    u_src, u_ry, u_sy, u_rz, u_sx, u_rx,
    c_src, c_ry, c_sy, c_rz, c_sx, c_rx, xg,
    g1, g2, g3, img, limg, vs,
    load_s, st_l, st_r, nat_s, nat_r, tq_s, tq_r, ex_s, ex_r, fw_s, fw_r,
    all_s, y_r, z_r, x_r, az_r, ay_r, pair_r, r8_r, c_s, c_r, r8f_s, r8f_r,
    im_s, im_r, if_s, if_r,
):
    ra, rb, c = lax.axis_index("rowa"), lax.axis_index("rowb"), lax.axis_index("col")
    y, z = rb % 4, rb // 4
    core, half = c % 2, c // 2
    mine, other = 2 * half, 2 - 2 * half
    sib, par, dia = c ^ 1, c ^ 2, c ^ 3

    def at_col(k):
        return (ra, rb, k)

    def at_y(d):
        return (ra, z * 4 + (y ^ d), c)

    def at_z(d):
        return (ra, (z ^ d) * 4 + y, c)

    def at_x(da, dc):
        return (ra ^ da, rb, c ^ dc)

    pending = []

    def send(a, b, s, r, dev):
        cp = pltpu.make_async_remote_copy(
            src_ref=a, dst_ref=b, send_sem=s, recv_sem=r, device_id=dev, device_id_type=MESH
        )
        cp.start()
        pending.append(cp)
        return cp

    def send_apart(*args):
        cp = send(*args)
        pending.pop()
        return cp

    class Waits:
        def __init__(self, whole, s, r):
            self.whole, self.s, self.r = whole, s, r

        def wait_send(self):
            pltpu.make_async_copy(self.whole, self.whole, self.s).wait()

        def wait_recv(self):
            pltpu.make_async_copy(self.whole, self.whole, self.r).wait()

    sent = [0]

    def sends(pairs, r, devs, whole):
        for (a, b), dev in zip(pairs, devs, strict=True):
            send_apart(a, b, all_s, r, dev)
        sent[0] += math.prod(whole.shape) // 1024
        return [Waits(whole, all_s, r)]

    three, seven = pl.ds(0, 3), pl.ds(0, 7)
    spot, spot2 = ra * 4 + c, ra * 2 + half
    pair = [at_col(sib)]

    def arrived(copies):
        for cp in copies:
            cp.wait_recv()

    XP = [(da, dc) for da in range(2) for dc in range(4) if (da, dc) != (0, 0)]

    own_start = pltpu.make_async_copy(start, rst.at[c], st_l)

    def load(i, q, o, n):
        cp = pltpu.make_async_copy(
            table.at[pl.ds(q * 2048 + o, n), :], tab.at[core, q, pl.ds(o, n), :], load_s.at[i]
        )
        cp.start()
        return cp

    loads = [load(p, other, 512 * p, 512) for p in range(4)]
    loads += [load(4 + i, q, 0, 2048) for i, q in enumerate((other + 1, mine, mine + 1))]
    own_start.start()

    barrier = pltpu.get_barrier_semaphore()
    for d in (1, 2, 3):
        pl.semaphore_signal(barrier, inc=1, device_id=at_y(d), device_id_type=MESH)
        pl.semaphore_signal(barrier, inc=1, device_id=at_z(d), device_id_type=MESH)
    for da, dc in XP:
        pl.semaphore_signal(barrier, inc=1, device_id=at_x(da, dc), device_id_type=MESH)

    def transpose_rows(q, first, blocks):
        def body(i, carry):
            o = pl.multiple_of(first + i * 256, 256)
            tt[q, :, pl.ds(o, 256)] = tab[core, q, pl.ds(o, 256), :].T
            return carry

        lax.fori_loop(0, blocks, body, 0)

    def columns(j):
        return pl.ds(sum(WIDTHS[:j]), WIDTHS[j])

    exchange = {}

    def send_chunk(j, k):
        w = columns(j)
        if j == CHUNKS - 1:
            for i, o, n in LAST[k]:
                part = pl.ds(o, n)
                send_apart(tt.at[other + k, w, part], r8.at[core, k, :, part], ex_s, r8_r.at[core, i], at_col(3 - 2 * half))
            return
        exchange[j, k] = [send_apart(tt.at[other + k, w], rt.at[k, w], ex_s, ex_r.at[j, k], at_col(par))]

    for p in range(4):
        loads[p].wait()
        transpose_rows(other, 512 * p, 2)
        if p == 0:
            pl.semaphore_wait(barrier, 13)
        o = pl.ds(512 * p, 512)
        send_apart(tt.at[other, columns(0), o], rt.at[0, columns(0), o], ex_s, ex_r.at[0, 0], at_col(par))
    whole = rt.at[0, columns(0)]
    exchange[0, 0] = [Waits(whole, ex_s, ex_r.at[0, 0])]
    nat = []
    for i, q in enumerate((mine, mine + 1, other, other + 1)):
        nat.append(
            send_apart(table.at[pl.ds(q * 2048, 2048), :], tab.at[core, q], nat_s, nat_r.at[i], at_col(sib))
        )
    pending.append(Waits(tab.at[0], nat_s, nat_s))
    loads[4].wait()
    transpose_rows(other + 1, 0, 8)
    for j, k in ((0, 1), (1, 0), (1, 1)):
        send_chunk(j, k)
    own_start.wait()
    starts = sends([(rst.at[c], rst.at[c])] * 3, st_r, [at_col(c ^ d) for d in (1, 2, 3)], rst.at[three])
    loads[5].wait()
    transpose_rows(mine, 0, 8)
    loads[6].wait()
    transpose_rows(mine + 1, 0, 8)
    tq = send(tt.at[mine + 1 - core], stt, tq_s, tq_r, at_col(sib))

    acc = jnp.zeros((128, 256), f32)
    for i, q in enumerate((mine, mine + 1, other, other + 1)):
        nat[i].wait_recv()

        def body(t, acc, i=i, q=q):
            o = pl.multiple_of(t * 512, 512)
            w = jnp.concatenate([tab[0, q, pl.ds(o, 512), :], tab[1, q, pl.ds(o, 512), :]], 1)
            h, l = split2(w)
            if i < 2:
                wh[i, pl.ds(o, 512), :] = h
                wl[i, pl.ds(o, 512), :] = l
            ah, al = split2(tt[q, :, pl.ds(o, 512)])
            both = dot(jnp.concatenate([ah, al], 0), h)
            return acc + (both[:128] + (both[128:] + dot(ah, l)))

        acc = lax.fori_loop(0, 4, body, acc)
    d_src[...] = acc.reshape(4, 4, 8, 256)

    def split_rows(block, ref):
        def body(i, carry):
            o = pl.multiple_of(i * 512, 512)
            h, l = split2(ref[:, pl.ds(o, 512)])
            ih[block, :, pl.ds(o, 512)] = h
            il[block, :, pl.ds(o, 512)] = l
            return carry

        lax.fori_loop(0, 4, body, 0)

    ys, zs = [at_y(d) for d in (1, 2, 3)], [at_z(d) for d in (1, 2, 3)]
    xs = [at_x(da, dc) for da, dc in XP]
    xs2 = [at_x(da, dc) for da, dc in ((0, 2), (1, 0), (1, 2))]

    def scattered(g, src, ry, sy, rz, sx, rx, gz, gy):
        hold = {}

        def stage0():
            hold["y"] = sends([(src.at[y ^ d], ry.at[d - 1]) for d in (1, 2, 3)], y_r.at[g], ys, ry)

        def stage1():
            arrived(hold["y"])
            sy[...] = src[y] + ry[0] + (ry[1] + ry[2])
            hold["z"] = sends([(sy.at[z ^ d], rz.at[d - 1]) for d in (1, 2, 3)], z_r.at[g], zs, rz)

        def stage2():
            arrived(hold["z"])
            total = sy[z] + rz[0] + (rz[1] + rz[2])
            sx[...] = total
            rx[spot2] = total
            hold["x"] = sends([(sx, rx.at[spot2])] * 3, x_r.at[g], xs2, rx.at[three])

        def stage3():
            arrived(hold["x"])
            gz[z] = rx[:2] + rx[2:]
            hold["az"] = sends([(gz.at[z], gz.at[z])] * 3, az_r.at[g], zs, gz.at[three])

        def stage4():
            arrived(hold["az"])
            hold["ay"] = sends([(gz, gy.at[core, y])] * 3, ay_r.at[g], ys, gy.at[core, three])
            gy[core, y] = gz[...]

        def stage5():
            arrived(hold["ay"])
            hold["pair"] = sends([(gy.at[core], gy.at[core])], pair_r.at[g], pair, gy.at[core])

        def stage6():
            arrived(hold["pair"])

        return stage0, stage1, stage2, stage3, stage4, stage5, stage6

    D = scattered(0, d_src, d_ry, d_sy, d_rz, d_sx, d_rx, d_gz, d_gy)
    E = scattered(1, e_src, e_ry, e_sy, e_rz, e_sx, e_rx, e_gz, e_gy)

    def f0(i):
        return sends([(f_src.at[i, y ^ d], f_ry.at[i, d - 1]) for d in (1, 2, 3)], y_r.at[2 + i], ys, f_ry.at[i])

    def f1(i, cps):
        arrived(cps)
        total = f_src[i, y] + f_ry[i, 0] + (f_ry[i, 1] + f_ry[i, 2])
        f_sy[i] = total
        f_rz[i, z] = total
        return sends([(f_sy.at[i], f_rz.at[i, z])] * 3, z_r.at[2 + i], zs, f_rz.at[i, three])

    def f2(i, cps):
        arrived(cps)
        total = (f_rz[i, 0] + f_rz[i, 1]) + (f_rz[i, 2] + f_rz[i, 3])
        f_sx[i] = total
        f_rx[i, spot2] = total
        return sends([(f_sx.at[i], f_rx.at[i, spot2])] * 3, x_r.at[2 + i], xs2, f_rx.at[i, three])

    def f3(i, cps):
        arrived(cps)
        f_gz[i] = f_rx[i, :2] + f_rx[i, 2:]
        out = sends([(f_gz.at[i], f_gy.at[i, core, y])] * 3, ay_r.at[2 + i], ys, f_gy.at[i, core, three])
        f_gy[i, core, y] = f_gz[i]
        return out

    def f4(i, cps):
        arrived(cps)
        whole = f_gy.at[i, core]
        return sends([(whole, whole)], pair_r.at[2 + i], pair, whole)

    T = (
        (t_src, t_ry, t_sy, t_rz, t_sx, t_rx),
        (u_src, u_ry, u_sy, u_rz, u_sx, u_rx),
    )

    def t0(i):
        src, ry = T[i][:2]
        ry[y] = src[...]
        return sends([(src, ry.at[y])] * 3, y_r.at[4 + i], ys, ry.at[three])

    def t1(i, cps):
        ry, sy, rz = T[i][1:4]
        arrived(cps)
        total = (ry[0] + ry[1]) + (ry[2] + ry[3])
        sy[...] = total
        rz[z] = total
        return sends([(sy, rz.at[z])] * 3, z_r.at[4 + i], zs, rz.at[three])

    def t2(i, cps):
        rz, sx, rx = T[i][3:]
        arrived(cps)
        total = (rz[0] + rz[1]) + (rz[2] + rz[3])
        sx[...] = total
        rx[spot] = total
        return sends([(sx, rx.at[spot])] * 7, x_r.at[4 + i], xs, rx.at[seven])

    def t2_equal(cps):
        arrived(cps)
        total = (t_rz[0] + t_rz[1]) + (t_rz[2] + t_rz[3])
        t_sx[...] = total
        t_rx[spot2] = total
        return sends([(t_sx, t_rx.at[spot2])] * 3, x_r.at[4], xs2, t_rx.at[three])

    def t3_equal(cps):
        arrived(cps)
        t_gy[core] = t_rx[:2] + t_rx[2:]
        whole = t_gy.at[core]
        return sends([(whole, whole)], pair_r.at[4], pair, whole)

    def on_core_1(stage):
        pl.when(core == 1)(stage)

    def c_send(a, b, i, devs):
        for dev in devs:
            send_apart(a, b, c_s, c_r.at[i], dev)

    def last_part(k, o, total):
        x = r8[:, k, :, pl.ds(o, 1024)].reshape(16, 1024)
        h = x.astype(bf16).astype(f32)
        both = jnp.concatenate([h, x - h], 0).astype(bf16)
        a, b = dot(both, wh[k, pl.ds(o, 1024), :]), dot(both, wl[k, pl.ds(o, 1024), :])
        return total + (a[:16] + ((a[16:] + b[:16]) + b[16:]))

    def c0():
        total = jnp.zeros((16, 256), f32)
        for k in range(2):
            for i, o, n in LAST[k]:
                for q in range(2):
                    Waits(r8.at[q, k, :, pl.ds(o, n)], ex_s, r8_r.at[q, i]).wait_recv()
                for first in range(o, o + n, 1024):
                    total = last_part(k, first, total)
        c_src[...] = total
        c_ry[y] = total
        c_send(c_src, c_ry.at[y], 0, ys)
        send_apart(r8.at[:, 0], r8.at[:, 0], r8f_s, r8f_r, at_col(sib))

    def c1():
        Waits(c_ry.at[three], c_s, c_r.at[0]).wait_recv()
        total = (c_ry[0] + c_ry[1]) + (c_ry[2] + c_ry[3])
        c_sy[...] = total
        c_rz[z] = total
        c_send(c_sy, c_rz.at[z], 1, zs)

    def c2():
        Waits(c_rz.at[three], c_s, c_r.at[1]).wait_recv()
        total = (c_rz[0] + c_rz[1]) + (c_rz[2] + c_rz[3])
        c_sx[...] = total
        c_rx[spot2] = total
        c_send(c_sx, c_rx.at[spot2], 2, xs)

    D[0]()
    split_rows(c, tt.at[mine + core])
    tq.wait_recv()
    split_rows(sib, stt)

    def chunk_part(j, k, first, count):
        w, n = columns(j), WIDTHS[j]

        def body(t, total):
            o = pl.multiple_of(first + t * 1024, 1024)
            x = rt[k, w, pl.ds(o, 1024)]
            h = x.astype(bf16).astype(f32)
            both = jnp.concatenate([h, x - h], 0).astype(bf16)
            a, b = dot(both, wh[k, pl.ds(o, 1024), :]), dot(both, wl[k, pl.ds(o, 1024), :])
            return total + (a[:n] + ((a[n:] + b[:n]) + b[n:]))

        zero = jnp.zeros((n, 256), f32)
        return body(0, zero) if count == 1 else lax.fori_loop(0, count, body, zero)

    def store_cover(r, k, x):
        for ref, part in zip((g1, g2, g3), split3(x)):
            ref[r : r + 128, k : k + 256] = part

    def issue(i):
        if i < 2 * CHUNKS:
            send_chunk(i // 2, i % 2)

    f, t = {}, {}
    for j in range(CHUNKS):
        w = columns(j)
        last = j == CHUNKS - 1
        if last:
            on_core_1(c0)
            break
        arrived(exchange[j, 0])
        total = chunk_part(j, 0, 0, 2)
        if j == 5:
            E[2]()
        arrived(exchange[j, 1])
        if j == 2:
            D[2]()
        if j == 6:
            f[0] = f2(0, f[0])
        for k in range(2):
            issue(2 * j + 4 + k)
        total = total + chunk_part(j, 1, 0, 2)
        if j < 6:
            for i in range(2):
                for n in range(2):
                    unit = total[8 * i : 8 * i + 8, 128 * n : 128 * n + 128]
                    if j < 4:
                        e_src[j, 2 * i + n] = unit
                    else:
                        f_src[j - 4, 2 * i + n] = unit
            if j >= 4:
                f[j - 4] = f0(j - 4)
        else:
            T[j - 6][0][...] = total
            t[j - 6] = t0(j - 6)
        send_apart(rt.at[1 - core, w], frt.at[w], fw_s, fw_r, at_col(sib))
        if j < 7:
            h, l = split2(rt[core, w, :])
            ih[par, w, :] = h
            il[par, w, :] = l
        if j == 1:
            D[1]()
        if j == 3:
            E[0]()
        if j == 4:
            D[3]()
            E[1]()
        if j == 5:
            D[4]()
            f[0] = f1(0, f[0])
        if j == 6:
            f[1] = f1(1, f[1])
            D[5]()
            E[3]()
    t[0] = t1(0, t[0])
    f[1] = f2(1, f[1])
    t[1] = t1(1, t[1])
    on_core_1(c1)
    t[0] = t2_equal(t[0])
    E[4]()
    f[0] = f3(0, f[0])
    f[1] = f3(1, f[1])
    t[1] = t2(1, t[1])
    on_core_1(c2)
    D[6]()
    for k in range(4):
        store_cover(128 * k, 256 * (k // 2), d_gy[k % 2, :, :, k // 2].reshape(128, 256))
    E[5]()
    f[0] = f4(0, f[0])
    f[1] = f4(1, f[1])
    t[0] = t3_equal(t[0])
    forwards = Waits(frt.at[:120], fw_s, fw_r)
    pending.append(forwards)
    forwards.wait_recv()
    to_core_0 = Waits(r8.at[:, 0], r8f_s, r8f_r)
    pl.when(core == 0)(to_core_0.wait_recv)
    frt[120:128, :] = r8[1 - core, core]
    rt[core, 120:128, :] = r8[core, core]
    split_rows(dia, frt)
    h, l = split2(rt[core, 112:128, :])
    ih[par, 112:128, :] = h
    il[par, 112:128, :] = l
    E[6]()
    for k in range(4):
        for r in range(4):
            for i in range(2):
                for n in range(2):
                    unit = e_gy[k % 2, r, 2 * i + n, k // 2]
                    xg[k, 16 * r + 8 * i : 16 * r + 8 * i + 8, 128 * n : 128 * n + 128] = unit
    arrived(starts)
    vectors = jnp.concatenate([rst[k] for k in range(4)], 1)
    for j in range(2):
        arrived(f[j])
        for k in range(4):
            for i in range(2):
                for n in range(2):
                    r = 64 + 16 * j + 8 * i
                    xg[k, r : r + 8, 128 * n : 128 * n + 128] = f_gy[j, k % 2, 2 * i + n, k // 2]
    arrived(t[0])
    for k in range(4):
        xg[k, columns(6), :] = t_gy[k % 2, k // 2]
    arrived(t[1])
    for k in range(4):
        xg[k, columns(7), :] = u_rx[k] + u_rx[4 + k]
    on_core_1(Waits(c_rx.at[three], c_s, c_r.at[2]).wait_recv)
    pl.when(core == 0)(Waits(c_rx, c_s, c_r.at[2]).wait_recv)
    for k in range(4):
        i = pl.ds(8 * (k % 2), 8)
        xg[k, 120:128, :] = c_rx[k // 2, i] + c_rx[2 + k // 2, i]
    across, below = xg[2:4].reshape(256, 256), xg[0:2].reshape(256, 256)
    upper, below = across + below.T, below + across.T
    store_cover(0, 256, upper[:128])
    store_cover(128, 256, upper[128:])
    store_cover(256, 0, below[:128])
    store_cover(384, 0, below[128:])

    def step(vectors):
        products = times_cover(vectors, g1, g2, g3)
        return orthonormal(outer_gram(products), products)

    vectors = lax.fori_loop(0, STEPS - 1, lambda i, v: step(v)[0], vectors)

    vh, vl = split2(vectors)
    vb = jnp.concatenate([vh, vl], 0)
    images = []
    for n in range(PIECES):
        o = pl.ds(IW * n, IW)
        h = jnp.concatenate([ih[k, :, o] for k in range(4)], 0)
        l = jnp.concatenate([il[k, :, o] for k in range(4)], 0)
        both = dot(vb, h)
        part = both[:16] + (both[16:] + dot(vh, l))
        img[n] = part
        limg[n, c] = part
        images.append(send_apart(img.at[n], limg.at[n, c], im_s.at[0], im_r.at[n], at_col(par)))
        send_apart(img.at[n], limg.at[n, c], im_s.at[1], im_r.at[PIECES], at_col(sib))
        if n == PIECES - 1:
            direct = send_apart(img.at[n], limg.at[n, c], im_s.at[2], im_r.at[PIECES + 1], at_col(dia))
    vectors, diagonal = step(vectors)
    for k in range(4):
        vs[k] = vectors[:, 128 * k : 128 * k + 128]
    right_o[...] = vs[c]
    eye = lax.broadcasted_iota(jnp.int32, (16, 128), 0) == lax.broadcasted_iota(jnp.int32, (16, 128), 1)
    str_o[...] = jnp.sum(jnp.where(eye, diagonal / rows_total, 0.0), 0, keepdims=True)[:, :16]

    for n in range(PIECES):
        images[n].wait_recv()
        if n < PIECES - 1:
            send_apart(limg.at[n, par], limg.at[n, par], if_s, if_r, at_col(sib))
    local, relays = Waits(img, im_s.at[1], im_r.at[PIECES]), Waits(img.at[: PIECES - 1], if_s, if_r)
    local.wait_recv()
    direct.wait_recv()
    relays.wait_recv()
    for n in range(PIECES):
        for k in range(4):
            left_o[:, 2048 * k + IW * n : 2048 * k + IW * n + IW] = limg[n, k]
    pending += [local, relays, direct, Waits(img, im_s.at[0], im_s.at[0])]
    pending.append(Waits(tab.at[0, :2], ex_s, ex_s))
    on_core_1(Waits(tab.at[0, :4, pl.ds(0, 2 * 52)], c_s, c_s).wait_send)
    on_core_1(to_core_0.wait_send)
    pending.append(Waits(tab.at[0, :4, pl.ds(0, 2 * sent[0])], all_s, all_s))
    for cp in pending:
        cp.wait_send()


def write_out(a, b, d, ao, bo, do, sem):
    copies = [pltpu.make_async_copy(x, o, sem.at[i]) for i, (x, o) in enumerate(((a, ao), (b, bo), (d, do)))]
    for cp in copies:
        cp.start()
    for cp in copies:
        cp.wait()


def scattered_scratch(*unit):
    V = pltpu.VMEM
    return [
        V((4, 4, *unit), f32),
        V((3, 4, *unit), f32),
        V((4, *unit), f32),
        V((3, *unit), f32),
        V(unit, f32),
        V((4, *unit), f32),
        V((4, 2, *unit), f32),
        V((2, 4, 4, 2, *unit), f32),
    ]


def on_device(rows_total, table, start):
    V, D = pltpu.VMEM, pltpu.SemaphoreType.DMA
    scratch = [
        V((2, 4, 2048, 128), f32),
        V((4, 128, 2048), f32),
        V((2, 128, 2048), f32),
        V((128, 2048), f32),
        V((128, 2048), f32),
        V((2, 2, 8, 2048), f32),
        V((2, 2048, 256), bf16),
        V((2, 2048, 256), bf16),
        V((4, 128, 2048), bf16),
        V((4, 128, 2048), bf16),
        V((4, 16, 128), f32),
        *scattered_scratch(8, 256),
        *scattered_scratch(8, 128),
        V((2, 4, 8, 128), f32),
        V((2, 3, 8, 128), f32),
        V((2, 8, 128), f32),
        V((2, 4, 8, 128), f32),
        V((2, 8, 128), f32),
        V((2, 4, 8, 128), f32),
        V((2, 2, 8, 128), f32),
        V((2, 2, 4, 2, 8, 128), f32),
        V((16, 256), f32),
        V((4, 16, 256), f32),
        V((16, 256), f32),
        V((4, 16, 256), f32),
        V((16, 256), f32),
        V((4, 16, 256), f32),
        V((2, 2, 16, 256), f32),
        V((8, 256), f32),
        V((4, 8, 256), f32),
        V((8, 256), f32),
        V((4, 8, 256), f32),
        V((8, 256), f32),
        V((8, 8, 256), f32),
        V((16, 256), f32),
        V((4, 16, 256), f32),
        V((16, 256), f32),
        V((4, 16, 256), f32),
        V((16, 256), f32),
        V((4, 16, 256), f32),
        V((4, 128, 256), f32),
        V((512, 512), bf16),
        V((512, 512), bf16),
        V((512, 512), bf16),
        V((PIECES, 16, IW), f32),
        V((PIECES, 4, 16, IW), f32),
        V((4, 16, 128), f32),
        D((7,)),
        D, D,
        D, D((4,)),
        D, D,
        D, D((CHUNKS - 1, 2)),
        D, D,
        D,
        D((6,)), D((6,)), D((6,)),
        D((2,)), D((4,)), D((5,)),
        D((2, 3)), D, D((3,)), D, D,
        D((3,)), D((PIECES + 2,)),
        D, D,
    ]
    table, start = (pltpu.with_memory_space_constraint(x, pltpu.HBM) for x in (table, start))
    results = pl.pallas_call(
        functools.partial(kernel, rows_total),
        out_shape=[V((16, 128), f32), V((16, 8192), f32), V((1, 16), f32)],
        in_specs=[pl.BlockSpec(memory_space=pltpu.HBM)] * 2,
        out_specs=[pl.BlockSpec(memory_space=V)] * 3,
        scratch_shapes=scratch,
        compiler_params=pltpu.CompilerParams(
            collective_id=0, has_side_effects=True, vmem_limit_bytes=48 * 1024 * 1024
        ),
    )(table, start)
    right, left, strengths = pl.pallas_call(
        write_out,
        out_shape=[jax.ShapeDtypeStruct(x.shape, f32) for x in results],
        in_specs=[pl.BlockSpec(memory_space=V)] * 3,
        out_specs=[pl.BlockSpec(memory_space=pl.ANY)] * 3,
        scratch_shapes=[D((3,))],
        compiler_params=pltpu.CompilerParams(vmem_limit_bytes=1024 * 1024),
    )(*results)
    return right, left, strengths.reshape(16)


def solution(mesh):
    rows_total = 8192 * mesh.shape["rowa"] * mesh.shape["rowb"]
    return jax.shard_map(
        functools.partial(on_device, rows_total),
        mesh=mesh,
        in_specs=(P(("rowa", "rowb"), "col"), P(None, "col")),
        out_specs=(P(None, "col"), P(None, ("rowa", "rowb")), P()),
        check_vma=False,
    )
```

```python
import functools
import math

import jax
import jax.numpy as jnp
from jax import lax
from jax.experimental import pallas as pl
from jax.experimental.pallas import tpu as pltpu
from jax.sharding import PartitionSpec as P

STEPS = 8
MESH = pl.DeviceIdType.MESH
f32 = jnp.float32
bf16 = jnp.bfloat16
WIDTHS = (16, 16, 16, 16, 16, 16, 16, 8, 8)
CHUNKS = len(WIDTHS)
LAST = (((0, 0, 2048),), ((1, 0, 1024), (2, 1024, 1024)))
PIECES = 8
IW = 2048 // PIECES


def dot(a, b):
    return lax.dot_general(a, b, (((1,), (0,)), ((), ())), preferred_element_type=f32)


def dot_nt(a, b):
    return lax.dot_general(a, b, (((1,), (1,)), ((), ())), preferred_element_type=f32)


def split2(x):
    h = x.astype(bf16)
    return h, (x - h.astype(f32)).astype(bf16)


def split3(x):
    h = x.astype(bf16)
    r = x - h.astype(f32)
    m = r.astype(bf16)
    return h, m, (r - m.astype(f32)).astype(bf16)


def times_cover(v, g1, g2, g3):
    h, m, l = split3(v)
    a = jnp.concatenate([h, m, l], 0)
    o1, o2, o3 = dot(a, g1[...]), dot(a[:32], g2[...]), dot(h, g3[...])
    return o1[:16] + (o1[16:32] + o2[:16]) + (o1[32:] + o2[16:] + o3)


def outer_gram(p):
    h, m, l = split3(p)
    a = jnp.concatenate([h, m, l], 0)
    o1, o2, o3 = dot_nt(a, h), dot_nt(a[:32], m), dot_nt(h, l)
    return o1[:16] + (o1[16:32] + o2[:16]) + (o1[32:] + o2[16:] + o3)


def orthonormal(gram, p):
    rows = lax.broadcasted_iota(jnp.int32, (16, 128), 0)
    cols = [jnp.broadcast_to(gram[:, k : k + 1], (16, 128)) for k in range(16)]
    tiles = [p[:, 128 * t : 128 * t + 128] for t in range(4)]
    pivots = jnp.zeros((16, 128), f32)
    for k in range(16):
        d = cols[k][k : k + 1, :]
        pivots = jnp.where(rows == k, d, pivots)
        if k < 15:
            m = jnp.where(rows > k, cols[k] * (1.0 / d), 0.0)
            for j in range(k + 1, 16):
                cols[j] = cols[j] - m * cols[j][k : k + 1, :]
            tiles = [t - m * t[k : k + 1, :] for t in tiles]
    s = jnp.sqrt(pivots)
    r = 1.0 / s
    return jnp.concatenate([t * r for t in tiles], 1), s


def kernel(
    rows_total,
    table, start, right_o, left_o, str_o,
    tab, tt, rt, stt, frt, r8, wh, wl, ih, il, rst,
    d_src, d_ry, d_sy, d_rz, d_sx, d_rx, d_gz, d_gy,
    e_src, e_ry, e_sy, e_rz, e_sx, e_rx, e_gz, e_gy,
    f_src, f_ry, f_sy, f_rz, f_sx, f_rx, f_gz, f_gy,
    t_src, t_ry, t_sy, t_rz, t_sx, t_rx,
    u_src, u_ry, u_sy, u_rz, u_sx, u_rx,
    c_src, c_ry, c_sy, c_rz, c_sx, c_rx, xg,
    g1, g2, g3, img, limg, vs,
    far, load_s, st_l, st_r, nat_s, nat_r, tq_s, tq_r, ex_s, ex_r, fw_s, fw_r,
    all_s, y_r, z_r, x_r, az_r, ay_r, pair_r, r8_r, c_s, c_r, r8f_s, r8f_r,
    im_s, im_r, if_s, if_r,
):
    ra, rb, c = lax.axis_index("rowa"), lax.axis_index("rowb"), lax.axis_index("col")
    y, z = rb % 4, rb // 4
    core, half = c % 2, c // 2
    mine, other = 2 * half, 2 - 2 * half
    sib, par, dia = c ^ 1, c ^ 2, c ^ 3

    def at_col(k):
        return (ra, rb, k)

    def at_y(d):
        return (ra, z * 4 + (y ^ d), c)

    def at_z(d):
        return (ra, (z ^ d) * 4 + y, c)

    def at_x(da, dc):
        return (ra ^ da, rb, c ^ dc)

    pending = []

    def send(a, b, s, r, dev):
        cp = pltpu.make_async_remote_copy(
            src_ref=a, dst_ref=b, send_sem=s, recv_sem=r, device_id=dev, device_id_type=MESH
        )
        cp.start()
        pending.append(cp)
        return cp

    def send_apart(*args):
        cp = send(*args)
        pending.pop()
        return cp

    class Waits:
        def __init__(self, whole, s, r):
            self.whole, self.s, self.r = whole, s, r

        def wait_send(self):
            pltpu.make_async_copy(self.whole, self.whole, self.s).wait()

        def wait_recv(self):
            pltpu.make_async_copy(self.whole, self.whole, self.r).wait()

    sent = [0]

    def sends(pairs, r, devs, whole):
        for (a, b), dev in zip(pairs, devs, strict=True):
            send_apart(a, b, all_s, r, dev)
        sent[0] += math.prod(whole.shape) // 1024
        return [Waits(whole, all_s, r)]

    three, seven = pl.ds(0, 3), pl.ds(0, 7)
    spot, spot2 = ra * 4 + c, ra * 2 + half
    pair = [at_col(sib)]

    def arrived(copies):
        for cp in copies:
            cp.wait_recv()

    XP = [(da, dc) for da in range(2) for dc in range(4) if (da, dc) != (0, 0)]

    own_start = pltpu.make_async_copy(start, rst.at[c], st_l)

    def load(i, q, o, n):
        cp = pltpu.make_async_copy(
            table.at[pl.ds(q * 2048 + o, n), :], tab.at[core, q, pl.ds(o, n), :], load_s.at[i]
        )
        cp.start()
        return cp

    loads = [load(p, other, 512 * p, 512) for p in range(4)]
    loads += [load(4 + i, q, 0, 2048) for i, q in enumerate((other + 1, mine, mine + 1))]
    own_start.start()

    def signal(sem, dev):
        pl.semaphore_signal(sem, inc=1, device_id=dev, device_id_type=MESH)

    barrier = pltpu.get_barrier_semaphore()
    near = [at_x(0, 1), at_x(0, 2), at_x(0, 3), at_x(1, 2), at_x(1, 3), at_y(1), at_y(3), at_z(1), at_z(3)]
    for dev in near:
        signal(barrier, dev)

    def transpose_rows(q, first, blocks):
        def body(i, carry):
            o = pl.multiple_of(first + i * 256, 256)
            tt[q, :, pl.ds(o, 256)] = tab[core, q, pl.ds(o, 256), :].T
            return carry

        lax.fori_loop(0, blocks, body, 0)

    def columns(j):
        return pl.ds(sum(WIDTHS[:j]), WIDTHS[j])

    exchange = {}

    def send_chunk(j, k):
        w = columns(j)
        if j == CHUNKS - 1:
            for i, o, n in LAST[k]:
                part = pl.ds(o, n)
                send_apart(tt.at[other + k, w, part], r8.at[core, k, :, part], ex_s, r8_r.at[core, i], at_col(3 - 2 * half))
            return
        exchange[j, k] = [send_apart(tt.at[other + k, w], rt.at[k, w], ex_s, ex_r.at[j, k], at_col(par))]

    for p in range(4):
        loads[p].wait()
        transpose_rows(other, 512 * p, 2)
        if p == 0:
            pl.semaphore_wait(barrier, len(near))
            for dev in (at_x(0, 2), at_y(1), at_z(1)):
                signal(far, dev)
        o = pl.ds(512 * p, 512)
        send_apart(tt.at[other, columns(0), o], rt.at[0, columns(0), o], ex_s, ex_r.at[0, 0], at_col(par))
    whole = rt.at[0, columns(0)]
    exchange[0, 0] = [Waits(whole, ex_s, ex_r.at[0, 0])]
    nat = []
    for i, q in enumerate((mine, mine + 1, other, other + 1)):
        nat.append(
            send_apart(table.at[pl.ds(q * 2048, 2048), :], tab.at[core, q], nat_s, nat_r.at[i], at_col(sib))
        )
    pending.append(Waits(tab.at[0], nat_s, nat_s))
    loads[4].wait()
    transpose_rows(other + 1, 0, 8)
    for j, k in ((0, 1), (1, 0), (1, 1)):
        send_chunk(j, k)
    own_start.wait()
    starts = sends([(rst.at[c], rst.at[c])] * 3, st_r, [at_col(c ^ d) for d in (1, 2, 3)], rst.at[three])
    loads[5].wait()
    transpose_rows(mine, 0, 8)
    loads[6].wait()
    transpose_rows(mine + 1, 0, 8)
    tq = send(tt.at[mine + 1 - core], stt, tq_s, tq_r, at_col(sib))

    acc = jnp.zeros((128, 256), f32)
    for i, q in enumerate((mine, mine + 1, other, other + 1)):
        nat[i].wait_recv()

        def body(t, acc, i=i, q=q):
            o = pl.multiple_of(t * 512, 512)
            w = jnp.concatenate([tab[0, q, pl.ds(o, 512), :], tab[1, q, pl.ds(o, 512), :]], 1)
            h, l = split2(w)
            if i < 2:
                wh[i, pl.ds(o, 512), :] = h
                wl[i, pl.ds(o, 512), :] = l
            ah, al = split2(tt[q, :, pl.ds(o, 512)])
            both = dot(jnp.concatenate([ah, al], 0), h)
            return acc + (both[:128] + (both[128:] + dot(ah, l)))

        acc = lax.fori_loop(0, 4, body, acc)
    d_src[...] = acc.reshape(4, 4, 8, 256)

    def split_rows(block, ref):
        def body(i, carry):
            o = pl.multiple_of(i * 512, 512)
            h, l = split2(ref[:, pl.ds(o, 512)])
            ih[block, :, pl.ds(o, 512)] = h
            il[block, :, pl.ds(o, 512)] = l
            return carry

        lax.fori_loop(0, 4, body, 0)

    ys, zs = [at_y(d) for d in (1, 2, 3)], [at_z(d) for d in (1, 2, 3)]
    xs = [at_x(da, dc) for da, dc in XP]
    xs2 = [at_x(da, dc) for da, dc in ((0, 2), (1, 0), (1, 2))]

    def scattered(g, src, ry, sy, rz, sx, rx, gz, gy):
        hold = {}

        def stage0():
            hold["y"] = sends([(src.at[y ^ d], ry.at[d - 1]) for d in (1, 2, 3)], y_r.at[g], ys, ry)

        def stage1():
            arrived(hold["y"])
            sy[...] = src[y] + ry[0] + (ry[1] + ry[2])
            hold["z"] = sends([(sy.at[z ^ d], rz.at[d - 1]) for d in (1, 2, 3)], z_r.at[g], zs, rz)

        def stage2():
            arrived(hold["z"])
            total = sy[z] + rz[0] + (rz[1] + rz[2])
            sx[...] = total
            rx[spot2] = total
            hold["x"] = sends([(sx, rx.at[spot2])] * 3, x_r.at[g], xs2, rx.at[three])

        def stage3():
            arrived(hold["x"])
            gz[z] = rx[:2] + rx[2:]
            hold["az"] = sends([(gz.at[z], gz.at[z])] * 3, az_r.at[g], zs, gz.at[three])

        def stage4():
            arrived(hold["az"])
            hold["ay"] = sends([(gz, gy.at[core, y])] * 3, ay_r.at[g], ys, gy.at[core, three])
            gy[core, y] = gz[...]

        def stage5():
            arrived(hold["ay"])
            hold["pair"] = sends([(gy.at[core], gy.at[core])], pair_r.at[g], pair, gy.at[core])

        def stage6():
            arrived(hold["pair"])

        return stage0, stage1, stage2, stage3, stage4, stage5, stage6

    D = scattered(0, d_src, d_ry, d_sy, d_rz, d_sx, d_rx, d_gz, d_gy)
    E = scattered(1, e_src, e_ry, e_sy, e_rz, e_sx, e_rx, e_gz, e_gy)

    def f0(i):
        return sends([(f_src.at[i, y ^ d], f_ry.at[i, d - 1]) for d in (1, 2, 3)], y_r.at[2 + i], ys, f_ry.at[i])

    def f1(i, cps):
        arrived(cps)
        total = f_src[i, y] + f_ry[i, 0] + (f_ry[i, 1] + f_ry[i, 2])
        f_sy[i] = total
        f_rz[i, z] = total
        return sends([(f_sy.at[i], f_rz.at[i, z])] * 3, z_r.at[2 + i], zs, f_rz.at[i, three])

    def f2(i, cps):
        arrived(cps)
        total = (f_rz[i, 0] + f_rz[i, 1]) + (f_rz[i, 2] + f_rz[i, 3])
        f_sx[i] = total
        f_rx[i, spot2] = total
        return sends([(f_sx.at[i], f_rx.at[i, spot2])] * 3, x_r.at[2 + i], xs2, f_rx.at[i, three])

    def f3(i, cps):
        arrived(cps)
        f_gz[i] = f_rx[i, :2] + f_rx[i, 2:]
        out = sends([(f_gz.at[i], f_gy.at[i, core, y])] * 3, ay_r.at[2 + i], ys, f_gy.at[i, core, three])
        f_gy[i, core, y] = f_gz[i]
        return out

    def f4(i, cps):
        arrived(cps)
        whole = f_gy.at[i, core]
        return sends([(whole, whole)], pair_r.at[2 + i], pair, whole)

    T = (
        (t_src, t_ry, t_sy, t_rz, t_sx, t_rx),
        (u_src, u_ry, u_sy, u_rz, u_sx, u_rx),
    )

    def t0(i):
        src, ry = T[i][:2]
        ry[y] = src[...]
        return sends([(src, ry.at[y])] * 3, y_r.at[4 + i], ys, ry.at[three])

    def t1(i, cps):
        ry, sy, rz = T[i][1:4]
        arrived(cps)
        total = (ry[0] + ry[1]) + (ry[2] + ry[3])
        sy[...] = total
        rz[z] = total
        return sends([(sy, rz.at[z])] * 3, z_r.at[4 + i], zs, rz.at[three])

    def t2(i, cps):
        rz, sx, rx = T[i][3:]
        arrived(cps)
        total = (rz[0] + rz[1]) + (rz[2] + rz[3])
        sx[...] = total
        rx[spot] = total
        return sends([(sx, rx.at[spot])] * 7, x_r.at[4 + i], xs, rx.at[seven])

    def on_core_1(stage):
        pl.when(core == 1)(stage)

    def c_send(a, b, i, devs):
        for dev in devs:
            send_apart(a, b, c_s, c_r.at[i], dev)

    def last_part(k, o, total):
        x = r8[:, k, :, pl.ds(o, 1024)].reshape(16, 1024)
        h = x.astype(bf16).astype(f32)
        both = jnp.concatenate([h, x - h], 0).astype(bf16)
        a, b = dot(both, wh[k, pl.ds(o, 1024), :]), dot(both, wl[k, pl.ds(o, 1024), :])
        return total + (a[:16] + ((a[16:] + b[:16]) + b[16:]))

    def c0():
        total = jnp.zeros((16, 256), f32)
        for k in range(2):
            for i, o, n in LAST[k]:
                for q in range(2):
                    Waits(r8.at[q, k, :, pl.ds(o, n)], ex_s, r8_r.at[q, i]).wait_recv()
                for first in range(o, o + n, 1024):
                    total = last_part(k, first, total)
        c_src[...] = total
        c_ry[y] = total
        c_send(c_src, c_ry.at[y], 0, ys)
        send_apart(r8.at[:, 0], r8.at[:, 0], r8f_s, r8f_r, at_col(sib))

    def c1():
        Waits(c_ry.at[three], c_s, c_r.at[0]).wait_recv()
        total = (c_ry[0] + c_ry[1]) + (c_ry[2] + c_ry[3])
        c_sy[...] = total
        c_rz[z] = total
        c_send(c_sy, c_rz.at[z], 1, zs)

    def c2():
        Waits(c_rz.at[three], c_s, c_r.at[1]).wait_recv()
        total = (c_rz[0] + c_rz[1]) + (c_rz[2] + c_rz[3])
        c_sx[...] = total
        c_rx[spot2] = total
        c_send(c_sx, c_rx.at[spot2], 2, xs)

    pl.semaphore_wait(far, 3)
    D[0]()
    split_rows(c, tt.at[mine + core])
    tq.wait_recv()
    split_rows(sib, stt)

    def chunk_part(j, k, first, count):
        w, n = columns(j), WIDTHS[j]

        def body(t, total):
            o = pl.multiple_of(first + t * 1024, 1024)
            x = rt[k, w, pl.ds(o, 1024)]
            h = x.astype(bf16).astype(f32)
            both = jnp.concatenate([h, x - h], 0).astype(bf16)
            a, b = dot(both, wh[k, pl.ds(o, 1024), :]), dot(both, wl[k, pl.ds(o, 1024), :])
            return total + (a[:n] + ((a[n:] + b[:n]) + b[n:]))

        zero = jnp.zeros((n, 256), f32)
        return body(0, zero) if count == 1 else lax.fori_loop(0, count, body, zero)

    def store_cover(r, k, x):
        for ref, part in zip((g1, g2, g3), split3(x)):
            ref[r : r + 128, k : k + 256] = part

    def issue(i):
        if i < 2 * CHUNKS:
            send_chunk(i // 2, i % 2)

    f, t = {}, {}
    for j in range(CHUNKS):
        w = columns(j)
        last = j == CHUNKS - 1
        if last:
            on_core_1(c0)
            break
        arrived(exchange[j, 0])
        total = chunk_part(j, 0, 0, 2)
        if j == 5:
            E[2]()
        arrived(exchange[j, 1])
        if j == 2:
            D[2]()
        if j == 6:
            f[0] = f2(0, f[0])
        for k in range(2):
            issue(2 * j + 4 + k)
        total = total + chunk_part(j, 1, 0, 2)
        if j < 6:
            for i in range(2):
                for n in range(2):
                    unit = total[8 * i : 8 * i + 8, 128 * n : 128 * n + 128]
                    if j < 4:
                        e_src[j, 2 * i + n] = unit
                    else:
                        f_src[j - 4, 2 * i + n] = unit
            if j >= 4:
                f[j - 4] = f0(j - 4)
        else:
            T[j - 6][0][...] = total
            t[j - 6] = t0(j - 6)
        send_apart(rt.at[1 - core, w], frt.at[w], fw_s, fw_r, at_col(sib))
        if j < 7:
            h, l = split2(rt[core, w, :])
            ih[par, w, :] = h
            il[par, w, :] = l
        if j == 1:
            D[1]()
        if j == 3:
            E[0]()
        if j == 4:
            D[3]()
            E[1]()
        if j == 5:
            D[4]()
            f[0] = f1(0, f[0])
        if j == 6:
            f[1] = f1(1, f[1])
            D[5]()
            E[3]()
    t[0] = t1(0, t[0])
    f[1] = f2(1, f[1])
    t[1] = t1(1, t[1])
    on_core_1(c1)
    t[0] = t2(0, t[0])
    E[4]()
    f[0] = f3(0, f[0])
    f[1] = f3(1, f[1])
    t[1] = t2(1, t[1])
    on_core_1(c2)
    D[6]()
    for k in range(4):
        store_cover(128 * k, 256 * (k // 2), d_gy[k % 2, :, :, k // 2].reshape(128, 256))
    E[5]()
    f[0] = f4(0, f[0])
    f[1] = f4(1, f[1])
    forwards = Waits(frt.at[:120], fw_s, fw_r)
    pending.append(forwards)
    forwards.wait_recv()
    to_core_0 = Waits(r8.at[:, 0], r8f_s, r8f_r)
    pl.when(core == 0)(to_core_0.wait_recv)
    frt[120:128, :] = r8[1 - core, core]
    rt[core, 120:128, :] = r8[core, core]
    split_rows(dia, frt)
    h, l = split2(rt[core, 112:128, :])
    ih[par, 112:128, :] = h
    il[par, 112:128, :] = l
    E[6]()
    for k in range(4):
        for r in range(4):
            for i in range(2):
                for n in range(2):
                    unit = e_gy[k % 2, r, 2 * i + n, k // 2]
                    xg[k, 16 * r + 8 * i : 16 * r + 8 * i + 8, 128 * n : 128 * n + 128] = unit
    arrived(starts)
    vectors = jnp.concatenate([rst[k] for k in range(4)], 1)
    for j in range(2):
        arrived(f[j])
        for k in range(4):
            for i in range(2):
                for n in range(2):
                    r = 64 + 16 * j + 8 * i
                    xg[k, r : r + 8, 128 * n : 128 * n + 128] = f_gy[j, k % 2, 2 * i + n, k // 2]
    for j in range(2):
        arrived(t[j])
        rx = T[j][5]
        for k in range(4):
            xg[k, columns(6 + j), :] = rx[k] + rx[4 + k]
    on_core_1(Waits(c_rx.at[three], c_s, c_r.at[2]).wait_recv)
    pl.when(core == 0)(Waits(c_rx, c_s, c_r.at[2]).wait_recv)
    for k in range(4):
        i = pl.ds(8 * (k % 2), 8)
        xg[k, 120:128, :] = c_rx[k // 2, i] + c_rx[2 + k // 2, i]
    across, below = xg[2:4].reshape(256, 256), xg[0:2].reshape(256, 256)
    upper, below = across + below.T, below + across.T
    store_cover(0, 256, upper[:128])
    store_cover(128, 256, upper[128:])
    store_cover(256, 0, below[:128])
    store_cover(384, 0, below[128:])

    def step(vectors):
        products = times_cover(vectors, g1, g2, g3)
        return orthonormal(outer_gram(products), products)

    vectors = lax.fori_loop(0, STEPS - 1, lambda i, v: step(v)[0], vectors)

    vh, vl = split2(vectors)
    vb = jnp.concatenate([vh, vl], 0)
    images = []
    for n in range(PIECES):
        o = pl.ds(IW * n, IW)
        h = jnp.concatenate([ih[k, :, o] for k in range(4)], 0)
        l = jnp.concatenate([il[k, :, o] for k in range(4)], 0)
        both = dot(vb, h)
        part = both[:16] + (both[16:] + dot(vh, l))
        img[n] = part
        limg[n, c] = part
        images.append(send_apart(img.at[n], limg.at[n, c], im_s.at[0], im_r.at[n], at_col(par)))
        send_apart(img.at[n], limg.at[n, c], im_s.at[1], im_r.at[PIECES], at_col(sib))
        if n == PIECES - 1:
            direct = send_apart(img.at[n], limg.at[n, c], im_s.at[2], im_r.at[PIECES + 1], at_col(dia))
    vectors, diagonal = step(vectors)
    for k in range(4):
        vs[k] = vectors[:, 128 * k : 128 * k + 128]
    right_o[...] = vs[c]
    eye = lax.broadcasted_iota(jnp.int32, (16, 128), 0) == lax.broadcasted_iota(jnp.int32, (16, 128), 1)
    str_o[...] = jnp.sum(jnp.where(eye, diagonal / rows_total, 0.0), 0, keepdims=True)[:, :16]

    for n in range(PIECES):
        images[n].wait_recv()
        if n < PIECES - 1:
            send_apart(limg.at[n, par], limg.at[n, par], if_s, if_r, at_col(sib))
    local, relays = Waits(img, im_s.at[1], im_r.at[PIECES]), Waits(img.at[: PIECES - 1], if_s, if_r)
    local.wait_recv()
    direct.wait_recv()
    relays.wait_recv()
    for n in range(PIECES):
        for k in range(4):
            left_o[:, 2048 * k + IW * n : 2048 * k + IW * n + IW] = limg[n, k]
    pending += [local, relays, direct, Waits(img, im_s.at[0], im_s.at[0])]
    pending.append(Waits(tab.at[0, :2], ex_s, ex_s))
    on_core_1(Waits(tab.at[0, :4, pl.ds(0, 2 * 52)], c_s, c_s).wait_send)
    on_core_1(to_core_0.wait_send)
    pending.append(Waits(tab.at[0, :4, pl.ds(0, 2 * sent[0])], all_s, all_s))
    for cp in pending:
        cp.wait_send()


def write_out(a, b, d, ao, bo, do, sem):
    copies = [pltpu.make_async_copy(x, o, sem.at[i]) for i, (x, o) in enumerate(((a, ao), (b, bo), (d, do)))]
    for cp in copies:
        cp.start()
    for cp in copies:
        cp.wait()


def scattered_scratch(*unit):
    V = pltpu.VMEM
    return [
        V((4, 4, *unit), f32),
        V((3, 4, *unit), f32),
        V((4, *unit), f32),
        V((3, *unit), f32),
        V(unit, f32),
        V((4, *unit), f32),
        V((4, 2, *unit), f32),
        V((2, 4, 4, 2, *unit), f32),
    ]


def on_device(rows_total, table, start):
    V, D = pltpu.VMEM, pltpu.SemaphoreType.DMA
    scratch = [
        V((2, 4, 2048, 128), f32),
        V((4, 128, 2048), f32),
        V((2, 128, 2048), f32),
        V((128, 2048), f32),
        V((128, 2048), f32),
        V((2, 2, 8, 2048), f32),
        V((2, 2048, 256), bf16),
        V((2, 2048, 256), bf16),
        V((4, 128, 2048), bf16),
        V((4, 128, 2048), bf16),
        V((4, 16, 128), f32),
        *scattered_scratch(8, 256),
        *scattered_scratch(8, 128),
        V((2, 4, 8, 128), f32),
        V((2, 3, 8, 128), f32),
        V((2, 8, 128), f32),
        V((2, 4, 8, 128), f32),
        V((2, 8, 128), f32),
        V((2, 4, 8, 128), f32),
        V((2, 2, 8, 128), f32),
        V((2, 2, 4, 2, 8, 128), f32),
        V((16, 256), f32),
        V((4, 16, 256), f32),
        V((16, 256), f32),
        V((4, 16, 256), f32),
        V((16, 256), f32),
        V((8, 16, 256), f32),
        V((8, 256), f32),
        V((4, 8, 256), f32),
        V((8, 256), f32),
        V((4, 8, 256), f32),
        V((8, 256), f32),
        V((8, 8, 256), f32),
        V((16, 256), f32),
        V((4, 16, 256), f32),
        V((16, 256), f32),
        V((4, 16, 256), f32),
        V((16, 256), f32),
        V((4, 16, 256), f32),
        V((4, 128, 256), f32),
        V((512, 512), bf16),
        V((512, 512), bf16),
        V((512, 512), bf16),
        V((PIECES, 16, IW), f32),
        V((PIECES, 4, 16, IW), f32),
        V((4, 16, 128), f32),
        pltpu.SemaphoreType.REGULAR,
        D((7,)),
        D, D,
        D, D((4,)),
        D, D,
        D, D((CHUNKS - 1, 2)),
        D, D,
        D,
        D((6,)), D((6,)), D((6,)),
        D((2,)), D((4,)), D((4,)),
        D((2, 3)), D, D((3,)), D, D,
        D((3,)), D((PIECES + 2,)),
        D, D,
    ]
    table, start = (pltpu.with_memory_space_constraint(x, pltpu.HBM) for x in (table, start))
    results = pl.pallas_call(
        functools.partial(kernel, rows_total),
        out_shape=[V((16, 128), f32), V((16, 8192), f32), V((1, 16), f32)],
        in_specs=[pl.BlockSpec(memory_space=pltpu.HBM)] * 2,
        out_specs=[pl.BlockSpec(memory_space=V)] * 3,
        scratch_shapes=scratch,
        compiler_params=pltpu.CompilerParams(
            collective_id=0, has_side_effects=True, vmem_limit_bytes=48 * 1024 * 1024
        ),
    )(table, start)
    right, left, strengths = pl.pallas_call(
        write_out,
        out_shape=[jax.ShapeDtypeStruct(x.shape, f32) for x in results],
        in_specs=[pl.BlockSpec(memory_space=V)] * 3,
        out_specs=[pl.BlockSpec(memory_space=pl.ANY)] * 3,
        scratch_shapes=[D((3,))],
        compiler_params=pltpu.CompilerParams(vmem_limit_bytes=1024 * 1024),
    )(*results)
    return right, left, strengths.reshape(16)


def solution(mesh):
    rows_total = 8192 * mesh.shape["rowa"] * mesh.shape["rowb"]
    return jax.shard_map(
        functools.partial(on_device, rows_total),
        mesh=mesh,
        in_specs=(P(("rowa", "rowb"), "col"), P(None, "col")),
        out_specs=(P(None, "col"), P(None, ("rowa", "rowb")), P()),
        check_vma=False,
    )
```

```python
import functools
import math

import jax
import jax.numpy as jnp
from jax import lax
from jax.experimental import pallas as pl
from jax.experimental.pallas import tpu as pltpu
from jax.sharding import PartitionSpec as P

STEPS = 8
MESH = pl.DeviceIdType.MESH
f32 = jnp.float32
bf16 = jnp.bfloat16
WIDTHS = (16, 16, 16, 16, 16, 16, 16, 8, 8)
CHUNKS = len(WIDTHS)
LAST = (((0, 0, 2048),), ((1, 0, 1024), (2, 1024, 1024)))
PIECES = 8
IW = 2048 // PIECES


def dot(a, b):
    return lax.dot_general(a, b, (((1,), (0,)), ((), ())), preferred_element_type=f32)


def dot_nt(a, b):
    return lax.dot_general(a, b, (((1,), (1,)), ((), ())), preferred_element_type=f32)


def split2(x):
    h = x.astype(bf16)
    return h, (x - h.astype(f32)).astype(bf16)


def split3(x):
    h = x.astype(bf16)
    r = x - h.astype(f32)
    m = r.astype(bf16)
    return h, m, (r - m.astype(f32)).astype(bf16)


def times_cover(v, g1, g2, g3):
    h, m, l = split3(v)
    a = jnp.concatenate([h, m, l], 0)
    o1, o2, o3 = dot(a, g1[...]), dot(a[:32], g2[...]), dot(h, g3[...])
    return o1[:16] + (o1[16:32] + o2[:16]) + (o1[32:] + o2[16:] + o3)


def outer_gram(p):
    h, m, l = split3(p)
    a = jnp.concatenate([h, m, l], 0)
    o1, o2, o3 = dot_nt(a, h), dot_nt(a[:32], m), dot_nt(h, l)
    return o1[:16] + (o1[16:32] + o2[:16]) + (o1[32:] + o2[16:] + o3)


def orthonormal(gram, p):
    rows = lax.broadcasted_iota(jnp.int32, (16, 128), 0)
    cols = [jnp.broadcast_to(gram[:, k : k + 1], (16, 128)) for k in range(16)]
    tiles = [p[:, 128 * t : 128 * t + 128] for t in range(4)]
    pivots = jnp.zeros((16, 128), f32)
    for k in range(16):
        d = cols[k][k : k + 1, :]
        pivots = jnp.where(rows == k, d, pivots)
        if k < 15:
            m = jnp.where(rows > k, cols[k] * (1.0 / d), 0.0)
            for j in range(k + 1, 16):
                cols[j] = cols[j] - m * cols[j][k : k + 1, :]
            tiles = [t - m * t[k : k + 1, :] for t in tiles]
    s = jnp.sqrt(pivots)
    r = 1.0 / s
    return jnp.concatenate([t * r for t in tiles], 1), s


def kernel(
    rows_total,
    table, start, right_o, left_o, str_o,
    tab, tt, rt, stt, frt, r8, wh, wl, ih, il, rst,
    d_src, d_ry, d_sy, d_rz, d_sx, d_rx, d_gz, d_gy,
    e_src, e_ry, e_sy, e_rz, e_sx, e_rx, e_gz, e_gy,
    f_src, f_ry, f_sy, f_rz, f_sx, f_rx, f_gz, f_gy,
    t_src, t_ry, t_sy, t_rz, t_sx, t_rx,
    u_src, u_ry, u_sy, u_rz, u_sx, u_rx,
    c_src, c_ry, c_sy, c_rz, c_sx, c_rx, xg,
    g1, g2, g3, img, limg, vs,
    far, load_s, st_l, st_r, nat_s, nat_r, tq_s, tq_r, ex_s, ex_r, fw_s, fw_r,
    all_s, y_r, z_r, x_r, az_r, ay_r, pair_r, r8_r, c_s, c_r, r8f_s, r8f_r,
    im_s, im_r, if_s, if_r,
):
    ra, rb, c = lax.axis_index("rowa"), lax.axis_index("rowb"), lax.axis_index("col")
    y, z = rb % 4, rb // 4
    core, half = c % 2, c // 2
    mine, other = 2 * half, 2 - 2 * half
    sib, par, dia = c ^ 1, c ^ 2, c ^ 3

    def at_col(k):
        return (ra, rb, k)

    def at_y(d):
        return (ra, z * 4 + (y ^ d), c)

    def at_z(d):
        return (ra, (z ^ d) * 4 + y, c)

    def at_x(da, dc):
        return (ra ^ da, rb, c ^ dc)

    pending = []

    def send(a, b, s, r, dev):
        cp = pltpu.make_async_remote_copy(
            src_ref=a, dst_ref=b, send_sem=s, recv_sem=r, device_id=dev, device_id_type=MESH
        )
        cp.start()
        pending.append(cp)
        return cp

    def send_apart(*args):
        cp = send(*args)
        pending.pop()
        return cp

    class Waits:
        def __init__(self, whole, s, r):
            self.whole, self.s, self.r = whole, s, r

        def wait_send(self):
            pltpu.make_async_copy(self.whole, self.whole, self.s).wait()

        def wait_recv(self):
            pltpu.make_async_copy(self.whole, self.whole, self.r).wait()

    sent = [0]

    def sends(pairs, r, devs, whole):
        for (a, b), dev in zip(pairs, devs, strict=True):
            send_apart(a, b, all_s, r, dev)
        sent[0] += math.prod(whole.shape) // 1024
        return [Waits(whole, all_s, r)]

    three, seven = pl.ds(0, 3), pl.ds(0, 7)
    spot, spot2 = ra * 4 + c, ra * 2 + half
    pair = [at_col(sib)]

    def arrived(copies):
        for cp in copies:
            cp.wait_recv()

    XP = [(da, dc) for da in range(2) for dc in range(4) if (da, dc) != (0, 0)]

    own_start = pltpu.make_async_copy(start, rst.at[c], st_l)

    def load(i, q, o, n):
        cp = pltpu.make_async_copy(
            table.at[pl.ds(q * 2048 + o, n), :], tab.at[core, q, pl.ds(o, n), :], load_s.at[i]
        )
        cp.start()
        return cp

    loads = [load(p, other, 512 * p, 512) for p in range(4)]
    loads += [load(4 + i, q, 0, 2048) for i, q in enumerate((other + 1, mine, mine + 1))]
    own_start.start()

    def signal(sem, dev):
        pl.semaphore_signal(sem, inc=1, device_id=dev, device_id_type=MESH)

    barrier = pltpu.get_barrier_semaphore()
    near = [at_x(0, 1), at_x(0, 2), at_x(0, 3), at_x(1, 2), at_x(1, 3), at_y(1), at_y(3), at_z(1), at_z(3)]
    for dev in near:
        signal(barrier, dev)

    def transpose_rows(q, first, blocks):
        def body(i, carry):
            o = pl.multiple_of(first + i * 256, 256)
            tt[q, :, pl.ds(o, 256)] = tab[core, q, pl.ds(o, 256), :].T
            return carry

        lax.fori_loop(0, blocks, body, 0)

    def columns(j):
        return pl.ds(sum(WIDTHS[:j]), WIDTHS[j])

    exchange = {}

    def send_chunk(j, k):
        w = columns(j)
        if j == CHUNKS - 1:
            for i, o, n in LAST[k]:
                part = pl.ds(o, n)
                send_apart(tt.at[other + k, w, part], r8.at[core, k, :, part], ex_s, r8_r.at[core, i], at_col(3 - 2 * half))
            return
        exchange[j, k] = [send_apart(tt.at[other + k, w], rt.at[k, w], ex_s, ex_r.at[j, k], at_col(par))]

    for p in range(4):
        loads[p].wait()
        transpose_rows(other, 512 * p, 2)
        if p == 0:
            pl.semaphore_wait(barrier, len(near))
            for dev in (at_x(0, 2), at_y(1), at_z(1)):
                signal(far, dev)
        o = pl.ds(512 * p, 512)
        send_apart(tt.at[other, columns(0), o], rt.at[0, columns(0), o], ex_s, ex_r.at[0, 0], at_col(par))
    whole = rt.at[0, columns(0)]
    exchange[0, 0] = [Waits(whole, ex_s, ex_r.at[0, 0])]
    nat = []
    for i, q in enumerate((mine, mine + 1, other, other + 1)):
        nat.append(
            send_apart(table.at[pl.ds(q * 2048, 2048), :], tab.at[core, q], nat_s, nat_r.at[i], at_col(sib))
        )
    pending.append(Waits(tab.at[0], nat_s, nat_s))
    loads[4].wait()
    transpose_rows(other + 1, 0, 8)
    for j, k in ((0, 1), (1, 0), (1, 1)):
        send_chunk(j, k)
    own_start.wait()
    starts = sends([(rst.at[c], rst.at[c])] * 3, st_r, [at_col(c ^ d) for d in (1, 2, 3)], rst.at[three])
    loads[5].wait()
    transpose_rows(mine, 0, 8)
    loads[6].wait()
    transpose_rows(mine + 1, 0, 8)
    tq = send(tt.at[mine + 1 - core], stt, tq_s, tq_r, at_col(sib))

    acc = jnp.zeros((128, 256), f32)
    for i, q in enumerate((mine, mine + 1, other, other + 1)):
        nat[i].wait_recv()

        def body(t, acc, i=i, q=q):
            o = pl.multiple_of(t * 512, 512)
            w = jnp.concatenate([tab[0, q, pl.ds(o, 512), :], tab[1, q, pl.ds(o, 512), :]], 1)
            h, l = split2(w)
            if i < 2:
                wh[i, pl.ds(o, 512), :] = h
                wl[i, pl.ds(o, 512), :] = l
            ah, al = split2(tt[q, :, pl.ds(o, 512)])
            both = dot(jnp.concatenate([ah, al], 0), h)
            return acc + (both[:128] + (both[128:] + dot(ah, l)))

        acc = lax.fori_loop(0, 4, body, acc)
    d_src[...] = acc.reshape(4, 4, 8, 256)

    def split_rows(block, ref):
        def body(i, carry):
            o = pl.multiple_of(i * 512, 512)
            h, l = split2(ref[:, pl.ds(o, 512)])
            ih[block, :, pl.ds(o, 512)] = h
            il[block, :, pl.ds(o, 512)] = l
            return carry

        lax.fori_loop(0, 4, body, 0)

    ys, zs = [at_y(d) for d in (1, 2, 3)], [at_z(d) for d in (1, 2, 3)]
    xs = [at_x(da, dc) for da, dc in XP]
    xs2 = [at_x(da, dc) for da, dc in ((0, 2), (1, 0), (1, 2))]

    def scattered(g, src, ry, sy, rz, sx, rx, gz, gy):
        hold = {}

        def stage0():
            hold["y"] = sends([(src.at[y ^ d], ry.at[d - 1]) for d in (1, 2, 3)], y_r.at[g], ys, ry)

        def stage1():
            arrived(hold["y"])
            sy[...] = src[y] + ry[0] + (ry[1] + ry[2])
            hold["z"] = sends([(sy.at[z ^ d], rz.at[d - 1]) for d in (1, 2, 3)], z_r.at[g], zs, rz)

        def stage2():
            arrived(hold["z"])
            total = sy[z] + rz[0] + (rz[1] + rz[2])
            sx[...] = total
            rx[spot2] = total
            hold["x"] = sends([(sx, rx.at[spot2])] * 3, x_r.at[g], xs2, rx.at[three])

        def stage3():
            arrived(hold["x"])
            gz[z] = rx[:2] + rx[2:]
            hold["az"] = sends([(gz.at[z], gz.at[z])] * 3, az_r.at[g], zs, gz.at[three])

        def stage4():
            arrived(hold["az"])
            hold["ay"] = sends([(gz, gy.at[core, y])] * 3, ay_r.at[g], ys, gy.at[core, three])
            gy[core, y] = gz[...]

        def stage5():
            arrived(hold["ay"])
            hold["pair"] = sends([(gy.at[core], gy.at[core])], pair_r.at[g], pair, gy.at[core])

        def stage6():
            arrived(hold["pair"])

        return stage0, stage1, stage2, stage3, stage4, stage5, stage6

    D = scattered(0, d_src, d_ry, d_sy, d_rz, d_sx, d_rx, d_gz, d_gy)
    E = scattered(1, e_src, e_ry, e_sy, e_rz, e_sx, e_rx, e_gz, e_gy)

    def f0(i):
        return sends([(f_src.at[i, y ^ d], f_ry.at[i, d - 1]) for d in (1, 2, 3)], y_r.at[2 + i], ys, f_ry.at[i])

    def f1(i, cps):
        arrived(cps)
        total = f_src[i, y] + f_ry[i, 0] + (f_ry[i, 1] + f_ry[i, 2])
        f_sy[i] = total
        f_rz[i, z] = total
        return sends([(f_sy.at[i], f_rz.at[i, z])] * 3, z_r.at[2 + i], zs, f_rz.at[i, three])

    def f2(i, cps):
        arrived(cps)
        total = (f_rz[i, 0] + f_rz[i, 1]) + (f_rz[i, 2] + f_rz[i, 3])
        f_sx[i] = total
        f_rx[i, spot2] = total
        return sends([(f_sx.at[i], f_rx.at[i, spot2])] * 3, x_r.at[2 + i], xs2, f_rx.at[i, three])

    def f3(i, cps):
        arrived(cps)
        f_gz[i] = f_rx[i, :2] + f_rx[i, 2:]
        out = sends([(f_gz.at[i], f_gy.at[i, core, y])] * 3, ay_r.at[2 + i], ys, f_gy.at[i, core, three])
        f_gy[i, core, y] = f_gz[i]
        return out

    def f4(i, cps):
        arrived(cps)
        whole = f_gy.at[i, core]
        return sends([(whole, whole)], pair_r.at[2 + i], pair, whole)

    T = (
        (t_src, t_ry, t_sy, t_rz, t_sx, t_rx),
        (u_src, u_ry, u_sy, u_rz, u_sx, u_rx),
    )

    def t0(i):
        src, ry = T[i][:2]
        ry[y] = src[...]
        return sends([(src, ry.at[y])] * 3, y_r.at[4 + i], ys, ry.at[three])

    def t1(i, cps):
        ry, sy, rz = T[i][1:4]
        arrived(cps)
        total = (ry[0] + ry[1]) + (ry[2] + ry[3])
        sy[...] = total
        rz[z] = total
        return sends([(sy, rz.at[z])] * 3, z_r.at[4 + i], zs, rz.at[three])

    def t2(i, cps):
        rz, sx, rx = T[i][3:]
        arrived(cps)
        total = (rz[0] + rz[1]) + (rz[2] + rz[3])
        sx[...] = total
        rx[spot] = total
        return sends([(sx, rx.at[spot])] * 7, x_r.at[4 + i], xs, rx.at[seven])

    def on_core_1(stage):
        pl.when(core == 1)(stage)

    def c_send(a, b, i, devs):
        for dev in devs:
            send_apart(a, b, c_s, c_r.at[i], dev)

    def last_part(k, o, total):
        x = r8[:, k, :, pl.ds(o, 1024)].reshape(16, 1024)
        h = x.astype(bf16).astype(f32)
        both = jnp.concatenate([h, x - h], 0).astype(bf16)
        a, b = dot(both, wh[k, pl.ds(o, 1024), :]), dot(both, wl[k, pl.ds(o, 1024), :])
        return total + (a[:16] + ((a[16:] + b[:16]) + b[16:]))

    def c0():
        total = jnp.zeros((16, 256), f32)
        for k in range(2):
            for i, o, n in LAST[k]:
                for q in range(2):
                    Waits(r8.at[q, k, :, pl.ds(o, n)], ex_s, r8_r.at[q, i]).wait_recv()
                for first in range(o, o + n, 1024):
                    total = last_part(k, first, total)
        c_src[...] = total
        c_ry[y] = total
        c_send(c_src, c_ry.at[y], 0, ys)
        send_apart(r8.at[:, 0], r8.at[:, 0], r8f_s, r8f_r, at_col(sib))

    def c1():
        Waits(c_ry.at[three], c_s, c_r.at[0]).wait_recv()
        total = (c_ry[0] + c_ry[1]) + (c_ry[2] + c_ry[3])
        c_sy[...] = total
        c_rz[z] = total
        c_send(c_sy, c_rz.at[z], 1, zs)

    def c2():
        Waits(c_rz.at[three], c_s, c_r.at[1]).wait_recv()
        total = (c_rz[0] + c_rz[1]) + (c_rz[2] + c_rz[3])
        c_sx[...] = total
        c_rx[spot2] = total
        c_send(c_sx, c_rx.at[spot2], 2, xs)

    pl.semaphore_wait(far, 3)
    D[0]()
    split_rows(c, tt.at[mine + core])
    tq.wait_recv()
    split_rows(sib, stt)

    def chunk_part(j, k, first, count):
        w, n = columns(j), WIDTHS[j]

        def body(t, total):
            o = pl.multiple_of(first + t * 1024, 1024)
            x = rt[k, w, pl.ds(o, 1024)]
            h = x.astype(bf16).astype(f32)
            both = jnp.concatenate([h, x - h], 0).astype(bf16)
            a, b = dot(both, wh[k, pl.ds(o, 1024), :]), dot(both, wl[k, pl.ds(o, 1024), :])
            return total + (a[:n] + ((a[n:] + b[:n]) + b[n:]))

        zero = jnp.zeros((n, 256), f32)
        return body(0, zero) if count == 1 else lax.fori_loop(0, count, body, zero)

    def store_cover(r, k, x):
        for ref, part in zip((g1, g2, g3), split3(x)):
            ref[r : r + 128, k : k + 256] = part

    def issue(i):
        if i < 2 * CHUNKS:
            send_chunk(i // 2, i % 2)

    f, t = {}, {}
    for j in range(CHUNKS):
        w = columns(j)
        last = j == CHUNKS - 1
        if last:
            on_core_1(c0)
            break
        arrived(exchange[j, 0])
        total = chunk_part(j, 0, 0, 2)
        if j == 5:
            E[2]()
        arrived(exchange[j, 1])
        if j == 2:
            D[2]()
        if j == 6:
            f[0] = f2(0, f[0])
        for k in range(2):
            issue(2 * j + 4 + k)
        total = total + chunk_part(j, 1, 0, 2)
        if j < 6:
            for i in range(2):
                for n in range(2):
                    unit = total[8 * i : 8 * i + 8, 128 * n : 128 * n + 128]
                    if j < 4:
                        e_src[j, 2 * i + n] = unit
                    else:
                        f_src[j - 4, 2 * i + n] = unit
            if j >= 4:
                f[j - 4] = f0(j - 4)
        else:
            T[j - 6][0][...] = total
            t[j - 6] = t0(j - 6)
        send_apart(rt.at[1 - core, w], frt.at[w], fw_s, fw_r, at_col(sib))
        if j < 7:
            h, l = split2(rt[core, w, :])
            ih[par, w, :] = h
            il[par, w, :] = l
        if j == 1:
            D[1]()
        if j == 3:
            E[0]()
        if j == 4:
            D[3]()
            E[1]()
        if j == 5:
            D[4]()
            f[0] = f1(0, f[0])
        if j == 6:
            f[1] = f1(1, f[1])
            D[5]()
            E[3]()
    t[0] = t1(0, t[0])
    f[1] = f2(1, f[1])
    t[1] = t1(1, t[1])
    on_core_1(c1)
    t[0] = t2(0, t[0])
    E[4]()
    f[0] = f3(0, f[0])
    f[1] = f3(1, f[1])
    t[1] = t2(1, t[1])
    on_core_1(c2)
    D[6]()
    for k in range(4):
        store_cover(128 * k, 256 * (k // 2), d_gy[k % 2, :, :, k // 2].reshape(128, 256))
    E[5]()
    f[0] = f4(0, f[0])
    f[1] = f4(1, f[1])
    forwards = Waits(frt.at[:120], fw_s, fw_r)
    pending.append(forwards)
    forwards.wait_recv()
    to_core_0 = Waits(r8.at[:, 0], r8f_s, r8f_r)
    pl.when(core == 0)(to_core_0.wait_recv)
    frt[120:128, :] = r8[1 - core, core]
    rt[core, 120:128, :] = r8[core, core]
    split_rows(dia, frt)
    h, l = split2(rt[core, 112:128, :])
    ih[par, 112:128, :] = h
    il[par, 112:128, :] = l
    E[6]()
    for k in range(4):
        for r in range(4):
            for i in range(2):
                for n in range(2):
                    unit = e_gy[k % 2, r, 2 * i + n, k // 2]
                    xg[k, 16 * r + 8 * i : 16 * r + 8 * i + 8, 128 * n : 128 * n + 128] = unit
    arrived(starts)
    vectors = jnp.concatenate([rst[k] for k in range(4)], 1)
    for j in range(2):
        arrived(f[j])
        for k in range(4):
            for i in range(2):
                for n in range(2):
                    r = 64 + 16 * j + 8 * i
                    xg[k, r : r + 8, 128 * n : 128 * n + 128] = f_gy[j, k % 2, 2 * i + n, k // 2]
    for j in range(2):
        arrived(t[j])
        rx = T[j][5]
        for k in range(4):
            xg[k, columns(6 + j), :] = rx[k] + rx[4 + k]
    on_core_1(Waits(c_rx.at[three], c_s, c_r.at[2]).wait_recv)
    pl.when(core == 0)(Waits(c_rx, c_s, c_r.at[2]).wait_recv)
    for k in range(4):
        i = pl.ds(8 * (k % 2), 8)
        xg[k, 120:128, :] = c_rx[k // 2, i] + c_rx[2 + k // 2, i]
    across, below = xg[2:4].reshape(256, 256), xg[0:2].reshape(256, 256)
    upper, below = across + below.T, below + across.T
    store_cover(0, 256, upper[:128])
    store_cover(128, 256, upper[128:])
    store_cover(256, 0, below[:128])
    store_cover(384, 0, below[128:])

    def step(vectors):
        products = times_cover(vectors, g1, g2, g3)
        return orthonormal(outer_gram(products), products)

    vectors = lax.fori_loop(0, STEPS - 1, lambda i, v: step(v)[0], vectors)

    vh, vl = split2(vectors)
    vb = jnp.concatenate([vh, vl], 0)
    images = []
    for n in range(PIECES):
        o = pl.ds(IW * n, IW)
        h = jnp.concatenate([ih[k, :, o] for k in range(4)], 0)
        l = jnp.concatenate([il[k, :, o] for k in range(4)], 0)
        both = dot(vb, h)
        part = both[:16] + (both[16:] + dot(vh, l))
        img[n] = part
        limg[n, c] = part
        images.append(send_apart(img.at[n], limg.at[n, c], im_s.at[0], im_r.at[n], at_col(par)))
        send_apart(img.at[n], limg.at[n, c], im_s.at[1], im_r.at[PIECES], at_col(sib))
        if n == PIECES - 1:
            direct = send_apart(img.at[n], limg.at[n, c], im_s.at[2], im_r.at[PIECES + 1], at_col(dia))
    vectors, diagonal = step(vectors)
    for k in range(4):
        vs[k] = vectors[:, 128 * k : 128 * k + 128]
    right_o[...] = vs[c]
    eye = lax.broadcasted_iota(jnp.int32, (16, 128), 0) == lax.broadcasted_iota(jnp.int32, (16, 128), 1)
    str_o[...] = jnp.sum(jnp.where(eye, diagonal / rows_total, 0.0), 0, keepdims=True)[:, :16]

    def put(n, k):
        left_o[:, pl.ds(pl.multiple_of(2048 * k + IW * n, IW), IW)] = limg[n, k]

    for n in range(PIECES):
        images[n].wait_recv()
        if n < PIECES - 1:
            send_apart(limg.at[n, par], limg.at[n, par], if_s, if_r, at_col(sib))
        put(n, c)
        put(n, par)
    local, relays = Waits(img, im_s.at[1], im_r.at[PIECES]), Waits(img.at[: PIECES - 1], if_s, if_r)
    local.wait_recv()
    direct.wait_recv()
    relays.wait_recv()
    for n in range(PIECES):
        put(n, sib)
        put(n, dia)
    pending += [local, relays, direct, Waits(img, im_s.at[0], im_s.at[0])]
    pending.append(Waits(tab.at[0, :2], ex_s, ex_s))
    on_core_1(Waits(tab.at[0, :4, pl.ds(0, 2 * 52)], c_s, c_s).wait_send)
    on_core_1(to_core_0.wait_send)
    pending.append(Waits(tab.at[0, :4, pl.ds(0, 2 * sent[0])], all_s, all_s))
    for cp in pending:
        cp.wait_send()


def write_out(a, b, d, ao, bo, do, sem):
    copies = [pltpu.make_async_copy(x, o, sem.at[i]) for i, (x, o) in enumerate(((a, ao), (b, bo), (d, do)))]
    for cp in copies:
        cp.start()
    for cp in copies:
        cp.wait()


def scattered_scratch(*unit):
    V = pltpu.VMEM
    return [
        V((4, 4, *unit), f32),
        V((3, 4, *unit), f32),
        V((4, *unit), f32),
        V((3, *unit), f32),
        V(unit, f32),
        V((4, *unit), f32),
        V((4, 2, *unit), f32),
        V((2, 4, 4, 2, *unit), f32),
    ]


def on_device(rows_total, table, start):
    V, D = pltpu.VMEM, pltpu.SemaphoreType.DMA
    scratch = [
        V((2, 4, 2048, 128), f32),
        V((4, 128, 2048), f32),
        V((2, 128, 2048), f32),
        V((128, 2048), f32),
        V((128, 2048), f32),
        V((2, 2, 8, 2048), f32),
        V((2, 2048, 256), bf16),
        V((2, 2048, 256), bf16),
        V((4, 128, 2048), bf16),
        V((4, 128, 2048), bf16),
        V((4, 16, 128), f32),
        *scattered_scratch(8, 256),
        *scattered_scratch(8, 128),
        V((2, 4, 8, 128), f32),
        V((2, 3, 8, 128), f32),
        V((2, 8, 128), f32),
        V((2, 4, 8, 128), f32),
        V((2, 8, 128), f32),
        V((2, 4, 8, 128), f32),
        V((2, 2, 8, 128), f32),
        V((2, 2, 4, 2, 8, 128), f32),
        V((16, 256), f32),
        V((4, 16, 256), f32),
        V((16, 256), f32),
        V((4, 16, 256), f32),
        V((16, 256), f32),
        V((8, 16, 256), f32),
        V((8, 256), f32),
        V((4, 8, 256), f32),
        V((8, 256), f32),
        V((4, 8, 256), f32),
        V((8, 256), f32),
        V((8, 8, 256), f32),
        V((16, 256), f32),
        V((4, 16, 256), f32),
        V((16, 256), f32),
        V((4, 16, 256), f32),
        V((16, 256), f32),
        V((4, 16, 256), f32),
        V((4, 128, 256), f32),
        V((512, 512), bf16),
        V((512, 512), bf16),
        V((512, 512), bf16),
        V((PIECES, 16, IW), f32),
        V((PIECES, 4, 16, IW), f32),
        V((4, 16, 128), f32),
        pltpu.SemaphoreType.REGULAR,
        D((7,)),
        D, D,
        D, D((4,)),
        D, D,
        D, D((CHUNKS - 1, 2)),
        D, D,
        D,
        D((6,)), D((6,)), D((6,)),
        D((2,)), D((4,)), D((4,)),
        D((2, 3)), D, D((3,)), D, D,
        D((3,)), D((PIECES + 2,)),
        D, D,
    ]
    table, start = (pltpu.with_memory_space_constraint(x, pltpu.HBM) for x in (table, start))
    results = pl.pallas_call(
        functools.partial(kernel, rows_total),
        out_shape=[V((16, 128), f32), V((16, 8192), f32), V((1, 16), f32)],
        in_specs=[pl.BlockSpec(memory_space=pltpu.HBM)] * 2,
        out_specs=[pl.BlockSpec(memory_space=V)] * 3,
        scratch_shapes=scratch,
        compiler_params=pltpu.CompilerParams(
            collective_id=0, has_side_effects=True, vmem_limit_bytes=48 * 1024 * 1024
        ),
    )(table, start)
    right, left, strengths = pl.pallas_call(
        write_out,
        out_shape=[jax.ShapeDtypeStruct(x.shape, f32) for x in results],
        in_specs=[pl.BlockSpec(memory_space=V)] * 3,
        out_specs=[pl.BlockSpec(memory_space=pl.ANY)] * 3,
        scratch_shapes=[D((3,))],
        compiler_params=pltpu.CompilerParams(vmem_limit_bytes=1024 * 1024),
    )(*results)
    return right, left, strengths.reshape(16)


def solution(mesh):
    rows_total = 8192 * mesh.shape["rowa"] * mesh.shape["rowb"]
    return jax.shard_map(
        functools.partial(on_device, rows_total),
        mesh=mesh,
        in_specs=(P(("rowa", "rowb"), "col"), P(None, "col")),
        out_specs=(P(None, "col"), P(None, ("rowa", "rowb")), P()),
        check_vma=False,
    )
```
